32 devices in a mesh: grp: 8 (over z, y), lane: 4 (over x, core).
Axes of the slice: x: 2, y: 2, z: 4, core: 2. Of those that a mesh axis runs over, the one named last changes fastest.
Arguments:
- grad_pooled: bfloat16 [4096, 16, 256], P(('grp', 'lane')), may hold values from -16 to 16
- bag_len: int32 [4096, 16], P(('grp', 'lane')), may hold values from 1 to 8
- lookup_slot: int32 [4096, 16, 8], P('grp', 'lane'), may hold values from -1 to 15, as said below
- slot_row: int32 [8, 4, 8, 2], P('grp', 'lane'), may hold values from 0 to 1023, as said below
- weights: float32 [16, 2048, 256], P('lane', 'grp'), may hold values from -6 to 6
- accum: float32 [16, 2048], P('lane', 'grp'), may hold values from 0.05 to 0.5
Outputs:
- new_weights: float32 [16, 2048, 256], P('lane', 'grp')
- new_accum: float32 [16, 2048], P('lane', 'grp')
The draws below stay inside these ranges and needn't reach their ends.
Inputs may be any that keep to these rules, and one draw needn't show every extreme that they name: `lookup_slot`: position j of bag (b, t) holds -1 when j >= bag_len[b, t] and otherwise a slot number s; the row slot_row[s // 2, t // 4, g, s % 2], with g the group of sample b, lies in local table t % 4. `slot_row`: several slots, also from different groups, may name the same row.
All inputs are finite; a program needn't handle non-finite values.
Results may differ from the reference program's by a relative error of at most 0.0035.
Values may be sent and summed in bfloat16 or wider, within the bound.
A program may use at most 64 MiB of HBM per device.

```python
import math
import jax
import jax.numpy as jnp
from jax import lax

EMBED = 256
TABLES_DEV = 4
BAG_MAX = 8
SLOTS_PEER = 2
BATCH_DEV = 128
ROWS_DEV = 256
TABLES = 16
BATCH = 4096
ROWS = 2048
SLOTS = 16
N_GRP = 8
N_LANE = 4
DEVICES = 32


def layout_keys(key):
    return jax.random.split(jax.random.fold_in(key, 913), 9)


def draw_grad_pooled(key, part):
    level_keys = jax.random.split(jax.random.fold_in(key, 421), 3)
    shape = (BATCH, TABLES, EMBED)
    level = jax.random.uniform(level_keys[0], (1, TABLES, 1), jnp.float32, -1.0, 1.0)
    base = 0.8 * jax.random.truncated_normal(level_keys[1], -4.0, 4.0, shape, jnp.float32)
    shared = 0.6 * jax.random.truncated_normal(level_keys[2], -3.0, 3.0, (1, TABLES, EMBED), jnp.float32)
    return ((base + shared) * jnp.exp(level)).astype(jnp.bfloat16)


def common_shift(key):
    keys = layout_keys(key)
    return jax.random.randint(keys[0], (N_LANE, N_GRP), 0, TABLES_DEV)


def common_lengths(key):
    keys = layout_keys(key)
    longest = jax.random.randint(keys[1], (DEVICES, 1, 1), 1, BAG_MAX + 1)
    raw_draw = jax.random.randint(keys[2], (DEVICES, BATCH_DEV, TABLES), 0, 1 << 20)
    lengths = (1 + raw_draw % longest).reshape(BATCH, TABLES)
    return lengths.at[0, 0].set(BAG_MAX).astype(jnp.int32)


def draw_bag_len(key, part):
    return common_lengths(key)


def draw_lookup_slot(key, part):
    keys = layout_keys(key)
    shift = common_shift(key)
    lengths = common_lengths(key)
    option_count = SLOTS // TABLES_DEV
    orders = jax.vmap(lambda one_key: jax.random.permutation(one_key, option_count))(jax.random.split(keys[3], N_LANE))
    shape = (BATCH, TABLES, BAG_MAX)
    first = jax.random.randint(keys[4], shape, 0, option_count)
    second = jax.random.randint(keys[5], shape, 0, option_count)
    third = jax.random.randint(keys[6], shape, 0, option_count)
    lowest = jnp.minimum(first, jnp.minimum(second, third))
    group_of = jnp.arange(BATCH, dtype=jnp.int32) // (BATCH_DEV * N_LANE)
    lane_of = jnp.arange(TABLES, dtype=jnp.int32) // TABLES_DEV
    table_local = jnp.arange(TABLES, dtype=jnp.int32) % TABLES_DEV
    picked = orders[lane_of[None, :, None], lowest]
    shift_here = shift[lane_of[None, :], group_of[:, None]]
    slot_number = picked * TABLES_DEV + ((table_local[None, :] - shift_here) % TABLES_DEV)[:, :, None]
    position = jnp.arange(BAG_MAX, dtype=jnp.int32)
    return jnp.where(position[None, None, :] < lengths[:, :, None], slot_number, -1).astype(jnp.int32)


def draw_slot_row(key, part):
    keys = layout_keys(key)
    shift = common_shift(key)
    slot_index = jnp.arange(SLOTS, dtype=jnp.int32).reshape(N_GRP, 1, 1, SLOTS_PEER)
    table_local = (slot_index + shift[None, :, :, None]) % TABLES_DEV
    shape = (N_GRP, N_LANE, N_GRP, SLOTS_PEER)
    hot_rows = jax.random.randint(keys[7], (N_GRP, N_LANE, 1, 8), 0, ROWS_DEV)
    sub_keys = jax.random.split(keys[8], 3)
    which = jax.random.randint(sub_keys[0], shape, 0, 8)
    hot_pick = jnp.take_along_axis(jnp.broadcast_to(hot_rows, (N_GRP, N_LANE, N_GRP, 8)), which, axis=3)
    drawn = jax.random.randint(sub_keys[1], shape, 0, ROWS_DEV)
    coin = jax.random.randint(sub_keys[2], shape, 0, 2)
    row_local = jnp.where(coin == 1, hot_pick, drawn)
    return (table_local * ROWS_DEV + row_local).astype(jnp.int32)


def block_levels(stream_key, shape, cuts, smallest, high):
    loudness, own = 1.0, jax.random.fold_in(stream_key, 6)
    for dim, parts in cuts:
        steps = jnp.exp(jax.random.uniform(jax.random.fold_in(own, dim), (parts,), jnp.float32, smallest / len(cuts), high / len(cuts)))
        loudness = loudness * jnp.repeat(steps, shape[dim] // parts).reshape([-1 if axis == dim else 1 for axis in range(len(shape))])
    return loudness


def noise(key, extent, width, bound, cuts=(), kind=jnp.bfloat16):
    values = jax.random.normal(key, extent, jnp.float32) * width
    if len(cuts) > 0:
        values = block_levels(key, extent, cuts, -0.22, 0.18) * values
    return jnp.clip(values, min=-bound, max=bound).astype(kind)


def setup_inputs(seed: int = 0) -> dict:
    seeds = jax.random.split(jax.random.key(seed), 7)
    grad_pooled = draw_grad_pooled(jax.random.fold_in(seeds[6], 71), 0)
    bag_len = draw_bag_len(jax.random.fold_in(seeds[6], 71), 0)
    lookup_slot = draw_lookup_slot(jax.random.fold_in(seeds[6], 71), 0)
    slot_row = draw_slot_row(jax.random.fold_in(seeds[6], 71), 0)
    weights = noise(seeds[4], (TABLES, ROWS, EMBED), 1.0, 6.0, ((0, 4), (1, 8)), jnp.float32)
    accum = jnp.clip(jnp.exp(math.log(0.5) - 2.3025851 * jax.random.uniform(seeds[5], (TABLES, ROWS), jnp.float32) ** block_levels(seeds[5], (TABLES, ROWS), ((0, 4), (1, 8)), -0.2, 0.2)), 0.05, 0.5)
    return {"grad_pooled": grad_pooled, "bag_len": bag_len, "lookup_slot": lookup_slot, "slot_row": slot_row, "weights": weights, "accum": accum}


def group_slot_sums(pieces):
    grad_block, length_block, slot_block = pieces
    scaled = (grad_block.astype(jnp.float32) / length_block.astype(jnp.float32)[:, :, None]).astype(jnp.bfloat16)
    values = scaled.astype(jnp.float32).reshape(N_LANE, BATCH_DEV, N_LANE, TABLES_DEV, 1, EMBED)
    slot_marks = slot_block.reshape(N_LANE, BATCH_DEV, N_LANE, TABLES_DEV, BAG_MAX)
    source_ids = jnp.arange(N_LANE, dtype=jnp.int32).reshape(N_LANE, 1, 1, 1, 1)
    target_ids = jnp.arange(N_LANE, dtype=jnp.int32).reshape(1, 1, N_LANE, 1, 1)
    dummy = N_LANE * N_LANE * SLOTS
    segment_ids = jnp.where(slot_marks >= 0, (source_ids * N_LANE + target_ids) * SLOTS + slot_marks, dummy)
    contrib = jnp.broadcast_to(values, (N_LANE, BATCH_DEV, N_LANE, TABLES_DEV, BAG_MAX, EMBED)).reshape(-1, EMBED)
    summed = jax.ops.segment_sum(contrib, segment_ids.reshape(-1).astype(jnp.int32), dummy + 1)
    partial_value = summed[:dummy].reshape(N_LANE, N_LANE, SLOTS, EMBED).astype(jnp.bfloat16)
    return lax.optimization_barrier(jnp.sum(partial_value.astype(jnp.float32), axis=0)).astype(jnp.bfloat16)

def reference(grad_pooled, bag_len, lookup_slot, slot_row, weights, accum):
    group_rows = N_LANE * BATCH_DEV
    slot_all = lax.map(group_slot_sums, (grad_pooled.reshape(N_GRP, group_rows, TABLES, EMBED), bag_len.reshape(N_GRP, group_rows, TABLES), lookup_slot.reshape(N_GRP, group_rows, TABLES, BAG_MAX)))
    local_index = jnp.transpose(slot_row, (2, 1, 0, 3))
    table_local = local_index // ROWS_DEV
    row_local = local_index % ROWS_DEV
    lane_ids = jnp.arange(N_LANE, dtype=jnp.int32).reshape(1, N_LANE, 1, 1)
    owner_ids = jnp.arange(N_GRP, dtype=jnp.int32).reshape(1, 1, N_GRP, 1)
    segment_ids = (lane_ids * TABLES_DEV + table_local) * ROWS + owner_ids * ROWS_DEV + row_local
    contrib = slot_all.astype(jnp.float32).reshape(-1, EMBED)
    row_grad = jax.ops.segment_sum(contrib, segment_ids.reshape(-1).astype(jnp.int32), TABLES * ROWS)
    row_grad = row_grad.reshape(TABLES, ROWS, EMBED)
    square_mean = lax.optimization_barrier(jnp.mean(row_grad * row_grad, axis=2))
    norm_total = EMBED * jnp.sum(square_mean)
    clip_limit = 0.5 * math.sqrt(DEVICES * SLOTS * EMBED)
    clip_factor = clip_limit / jnp.maximum(jnp.sqrt(norm_total), clip_limit)
    new_accum = accum + clip_factor * clip_factor * square_mean
    new_weights = weights - 0.3 * clip_factor * row_grad / (jnp.sqrt(new_accum)[:, :, None] + 1e-06)
    return (new_weights, new_accum)
```

```python
import functools
import math

import jax
import jax.numpy as jnp
from jax import lax
from jax.experimental import pallas as pl
from jax.experimental.pallas import tpu as pltpu
from jax.sharding import PartitionSpec as P

MESH = pl.DeviceIdType.MESH
LEARN_RATE = 0.3
EPSILON = 1e-06
F32 = jnp.float32
BF16 = jnp.bfloat16


def each(count, body):
    if count <= 64:
        for i in range(count):
            body(i)
    else:

        def step(i, carry):
            body(i)
            return carry

        lax.fori_loop(0, count, step, 0)


def iota(shape, dim):
    return lax.broadcasted_iota(jnp.int32, shape, dim)


def kernel(
    groups,
    lanes,
    place_base,
    accum_base,
    grad_hbm,
    len_hbm,
    look_hbm,
    slot_hbm,
    accum_hbm,
    packed,
    grad_in,
    grad_f32,
    grad_t,
    len_v,
    marks,
    marks_in,
    marks_out,
    slot_v,
    accum_v,
    part,
    recv,
    incoming,
    norm_out,
    norm_in,
    load_sem,
    look_sem,
    a_send,
    a_recv,
    b_send,
    b_recv,
    c_send,
    c_recv,
):
    devices = groups * lanes
    per_peer, embed = recv.shape[1], recv.shape[2]
    slots = groups * per_peer
    tables_all, batch = grad_t.shape[0], grad_t.shape[1]
    tables = tables_all // lanes
    depth = marks.shape[2]
    rows = accum_v.shape[1]
    grp = lax.axis_index("grp")
    lane = lax.axis_index("lane")
    me = grp * lanes + lane
    sign = 2 * (grp // (groups // 2)) - 1

    lane_steps = [(dx, dc) for dx in range(lanes // 2) for dc in range(2)]

    def lane_peer(step, sign):
        dx, dc = step
        half = lanes // 2
        chip = (lane // 2 + sign * dx + half) % half
        return chip * 2 + (lane % 2 + dc) % 2

    def partial_of(m):
        highs, lows = [], []
        for t in range(tables):
            mark = marks[m, t].astype(F32)
            count = jnp.zeros((slots, batch), F32)
            for j in range(depth):
                count += jnp.where(mark[j : j + 1, :] == number, 1.0, 0.0)
            length = len_v[pl.ds(m * tables + t, 1), :].astype(F32)
            factor = count / length
            high = factor.astype(BF16)
            highs.append(high)
            lows.append((factor - high.astype(F32)).astype(BF16))
        factors = jnp.concatenate(
            [jnp.concatenate(highs, axis=1), jnp.concatenate(lows, axis=1)], axis=0
        )
        values = grad_t[pl.ds(m * tables, tables)].reshape(tables * batch, embed)
        both = jnp.dot(factors, values, preferred_element_type=F32)
        return both[:slots] + both[slots:]

    barrier = pltpu.get_barrier_semaphore()

    def greet(i):
        far = (me + sign * (i + 1) + devices) % devices
        pl.semaphore_signal(
            barrier, inc=1, device_id=(far // lanes, far % lanes), device_id_type=MESH
        )

    look_copies = []
    for k, step in enumerate(lane_steps):
        q = lane_peer(step, 1)
        src = look_hbm.at[:, :, pl.ds(pl.multiple_of(q * batch, batch), batch)]
        look_copies.append(pltpu.make_async_copy(src, marks_in.at[k], look_sem.at[k]))
        look_copies[-1].start()
    grad_copy = pltpu.make_async_copy(grad_hbm, grad_in, load_sem.at[0])
    grad_copy.start()
    if devices <= 64:
        for i in range(devices - 1):
            greet(i)
    else:
        each(devices - 1, greet)
    small_copies = [
        pltpu.make_async_copy(len_hbm, len_v, load_sem.at[1]),
        pltpu.make_async_copy(slot_hbm, slot_v, load_sem.at[2]),
        pltpu.make_async_copy(accum_hbm, accum_v, load_sem.at[3]),
    ]
    for copy in small_copies:
        copy.start()
    for copy in look_copies:
        copy.wait()
    for k in range(1, lanes):
        marks_out[k - 1] = marks_in[k].astype(F32).astype(marks_out.dtype)
    pl.semaphore_wait(barrier, devices - 1)

    a_copies = []
    for k, step in enumerate(lane_steps[1:], 1):
        copy = pltpu.make_async_remote_copy(
            src_ref=marks_out.at[k - 1],
            dst_ref=marks.at[lane],
            send_sem=a_send.at[k - 1],
            recv_sem=a_recv.at[k - 1],
            device_id=(grp, lane_peer(step, 1)),
            device_id_type=MESH,
        )
        copy.start()
        a_copies.append(copy)

    grad_copy.wait()
    for c in range(embed // 128):
        grad_f32[c] = grad_in[:, c * 128 : (c + 1) * 128].astype(F32)
    for t in range(tables_all):
        for c in range(embed // 128):
            grad_t[t, :, c * 128 : (c + 1) * 128] = grad_f32[
                c, pl.ds(t, batch, stride=tables_all), :
            ].astype(BF16)
    for copy in small_copies:
        copy.wait()

    marks[lane] = marks_in[0].astype(F32).astype(marks.dtype)
    number = iota((slots, batch), 0).astype(F32)
    far_first = list(range(1, groups)) + [0]

    for k, step in enumerate(lane_steps):
        m = lane_peer(step, -1)
        if k > 0:
            a_copies[k - 1].wait_recv()
        total = partial_of(m)
        for p in range(groups):
            part[m, p] = total[p * per_peer : (p + 1) * per_peer].astype(BF16)

        def send(p):
            pltpu.make_async_remote_copy(
                src_ref=part.at[m, p],
                dst_ref=recv.at[me],
                send_sem=b_send,
                recv_sem=b_recv,
                device_id=(p, m),
                device_id_type=MESH,
            ).start()

        if groups <= 64:
            for dp in far_first:
                if k == 0 and dp == 0:
                    pltpu.make_async_copy(part.at[m, grp], recv.at[me], b_recv).start()
                else:
                    send((grp + sign * dp + groups) % groups)
        else:
            each(groups - 1, lambda i: send((grp + i + 1) % groups))
            if k == 0:
                pltpu.make_async_copy(part.at[m, grp], recv.at[me], b_recv).start()
            else:
                send(grp)

    slot_f = slot_v[...].astype(F32)
    which = iota((slots, groups), 0)
    column_pick = jnp.zeros((slots, groups), F32)
    for k in range(per_peer):
        column_pick = jnp.where(which % per_peer == k, slot_f[k : k + 1, :], column_pick)
    column_pick = jnp.where(which // per_peer == iota((slots, groups), 1), column_pick, 0.0)
    target_col = jnp.sum(column_pick, axis=1, keepdims=True)
    i_id, j_id = iota((slots, slots), 0), iota((slots, slots), 1)
    target_row = jnp.sum(jnp.where(i_id == j_id, target_col, 0.0), axis=0, keepdims=True)
    same = target_col == target_row
    first_col = jnp.sum(jnp.where(same & (j_id < i_id), 1.0, 0.0), axis=1, keepdims=True) == 0.0
    first_row = jnp.sum(jnp.where(same & (i_id < j_id), 1.0, 0.0), axis=0, keepdims=True) == 0.0
    place_row = jnp.where(first_row, target_row, -1.0)
    packed[place_base : place_base + 1, :slots] = place_row
    same_w = jnp.where(same, 1.0, 0.0).astype(BF16)

    hits = []
    accum_col = jnp.zeros((slots, 1), F32)
    for t in range(tables):
        hit = target_col == (iota((slots, rows), 1) + t * rows).astype(F32)
        hits.append(hit)
        accum_col += jnp.sum(
            jnp.where(hit, accum_v[t : t + 1, :], 0.0), axis=1, keepdims=True
        )

    pltpu.make_async_copy(recv, recv, b_recv).wait()
    for g in range(groups):
        group_sum = recv[g * lanes].astype(F32)
        for q in range(1, lanes):
            group_sum += recv[g * lanes + q].astype(F32)
        incoming[g * per_peer : (g + 1) * per_peer, :] = group_sum
    grads = jnp.dot(same_w, incoming[...].astype(BF16), preferred_element_type=F32)
    square_col = jnp.sum(grads * grads, axis=1, keepdims=True) * (1.0 / embed)
    square_first = jnp.where(first_col, square_col, 0.0)
    local = embed * jnp.sum(square_first, axis=0, keepdims=True)
    norm_out[...] = jnp.broadcast_to(local, (1, 128))

    def tell(far):
        pltpu.make_async_remote_copy(
            src_ref=norm_out,
            dst_ref=norm_in.at[me],
            send_sem=c_send,
            recv_sem=c_recv,
            device_id=(far // lanes, far % lanes),
            device_id_type=MESH,
        ).start()

    if devices <= 64:
        for d in range(1, devices):
            tell((me + sign * d + devices) % devices)
    else:
        each(devices - 1, lambda i: tell((me + i + 1) % devices))
    pltpu.make_async_copy(norm_out, norm_in.at[me], c_recv).start()

    square_rows = [
        jnp.sum(jnp.where(hit, square_first, 0.0), axis=0, keepdims=True) for hit in hits
    ]
    for copy in a_copies:
        copy.wait_send()
    sent = recv.at[pl.ds(0, devices - 1)]
    pltpu.make_async_copy(sent, sent, b_send).wait()

    pltpu.make_async_copy(norm_in, norm_in, c_recv).wait()
    norm_total = jnp.sum(norm_in[...], axis=0)[:, :1]
    clip_limit = 0.5 * math.sqrt(devices * slots * embed)
    clip = clip_limit / jnp.maximum(jnp.sqrt(norm_total), clip_limit)
    for t in range(tables):
        packed[accum_base + t : accum_base + t + 1, :rows] = accum_v[t : t + 1, :] + clip * clip * square_rows[t]
    new_accum_col = accum_col + clip * clip * square_col
    delta = LEARN_RATE * clip * grads / (jnp.sqrt(new_accum_col) + EPSILON)
    packed[:slots, :embed] = delta
    told = norm_in.at[pl.ds(0, devices - 1)]
    pltpu.make_async_copy(told, told, c_send).wait()


def update_kernel(
    chunk, slots, place_base, accum_base, weights, packed, wout, aout, held, accum, sems, accum_sem
):
    accum[...] = packed[accum_base : accum_base + accum.shape[0], : accum.shape[1]]
    accum_copy = pltpu.make_async_copy(accum, aout, accum_sem)
    accum_copy.start()
    delta = packed[:slots, : weights.shape[2]]
    high = delta.astype(BF16)
    deltas = jnp.concatenate([high, (delta - high.astype(F32)).astype(BF16)], axis=0)
    place_row = packed[place_base : place_base + 1, :slots]
    place_row = jnp.concatenate([place_row, place_row], axis=1)
    tables, rows = weights.shape[0], weights.shape[1]
    copies = []
    for t in range(tables):
        for c in range(0, rows, chunk):
            row_id = (iota((chunk, 1), 0) + (t * rows + c)).astype(F32)
            place = jnp.where(row_id == place_row, 1.0, 0.0).astype(BF16)
            held[t, c : c + chunk] = weights[t, c : c + chunk] - jnp.dot(
                place, deltas, preferred_element_type=F32
            )
            copies.append(
                pltpu.make_async_copy(
                    held.at[t, pl.ds(c, chunk)],
                    wout.at[t, pl.ds(c, chunk)],
                    sems.at[len(copies)],
                )
            )
            copies[-1].start()
    for copy in copies:
        copy.wait()
    accum_copy.wait()


def per_device(groups, lanes, grad_pooled, bag_len, lookup_slot, slot_row, weights, accum):
    batch, tables_all, embed = grad_pooled.shape
    samples, tables, depth = lookup_slot.shape
    rows = accum.shape[1]
    per_peer = slot_row.shape[3]
    devices = groups * lanes
    slots = groups * per_peer
    mark_type = BF16 if slots <= 256 else F32
    place_base = -(-slots // 8) * 8
    accum_base = place_base + 8
    packed_shape = (accum_base + -(-tables // 8) * 8, max(embed, rows, slots))
    anywhere = pl.BlockSpec(memory_space=pl.ANY)
    vmem = pl.BlockSpec(memory_space=pltpu.VMEM)
    packed = pl.pallas_call(
        functools.partial(kernel, groups, lanes, place_base, accum_base),
        out_shape=jax.ShapeDtypeStruct(packed_shape, F32),
        in_specs=[pl.BlockSpec(memory_space=pltpu.HBM)] * 5,
        out_specs=vmem,
        cost_estimate=pl.CostEstimate(
            flops=8 * slots * batch * tables_all * embed,
            bytes_accessed=32 * batch * tables_all * embed,
            transcendentals=0,
        ),
        scratch_shapes=[
            pltpu.VMEM((batch * tables_all, embed), BF16),
            pltpu.VMEM((embed // 128, batch * tables_all, 128), F32),
            pltpu.VMEM((tables_all, batch, embed), BF16),
            pltpu.VMEM((tables_all, batch), jnp.int32),
            pltpu.VMEM((lanes, tables, depth, batch), mark_type),
            pltpu.VMEM((lanes, tables, depth, batch), jnp.int32),
            pltpu.VMEM((lanes - 1, tables, depth, batch), mark_type),
            pltpu.VMEM((per_peer, groups), jnp.int32),
            pltpu.VMEM((tables, rows), F32),
            pltpu.VMEM((lanes, groups, per_peer, embed), BF16),
            pltpu.VMEM((devices, per_peer, embed), BF16),
            pltpu.VMEM((slots, embed), F32),
            pltpu.VMEM((1, 128), F32),
            pltpu.VMEM((devices, 1, 128), F32),
            pltpu.SemaphoreType.DMA((4,)),
            pltpu.SemaphoreType.DMA((lanes,)),
            pltpu.SemaphoreType.DMA((lanes - 1,)),
            pltpu.SemaphoreType.DMA((lanes - 1,)),
            pltpu.SemaphoreType.DMA,
            pltpu.SemaphoreType.DMA,
            pltpu.SemaphoreType.DMA,
            pltpu.SemaphoreType.DMA,
        ],
        compiler_params=pltpu.CompilerParams(
            collective_id=0, has_side_effects=True, vmem_limit_bytes=32 << 20
        ),
    )(
        *(
            pltpu.with_memory_space_constraint(operand, pltpu.HBM)
            for operand in (
                grad_pooled.reshape(batch * tables_all, embed),
                bag_len.T,
                jnp.transpose(lookup_slot, (1, 2, 0)),
                slot_row.reshape(groups, per_peer).T,
                accum,
            )
        )
    )
    chunk = min(rows, 128)
    return pl.pallas_call(
        functools.partial(update_kernel, chunk, slots, place_base, accum_base),
        out_shape=(
            jax.ShapeDtypeStruct(weights.shape, F32),
            jax.ShapeDtypeStruct(accum.shape, F32),
        ),
        in_specs=[vmem, vmem],
        out_specs=(anywhere, anywhere),
        scratch_shapes=[
            pltpu.VMEM(weights.shape, F32),
            pltpu.VMEM(accum.shape, F32),
            pltpu.SemaphoreType.DMA((tables * (rows // chunk),)),
            pltpu.SemaphoreType.DMA,
        ],
        compiler_params=pltpu.CompilerParams(vmem_limit_bytes=8 << 20),
    )(weights, packed)


def solution(mesh):
    placed = (
        P(("grp", "lane"), None, None),
        P(("grp", "lane"), None),
        P("grp", "lane", None),
        P("grp", "lane", None, None),
        P("lane", "grp", None),
        P("lane", "grp"),
    )
    return jax.shard_map(
        functools.partial(per_device, mesh.shape["grp"], mesh.shape["lane"]),
        mesh=mesh,
        in_specs=placed,
        out_specs=(P("lane", "grp", None), P("lane", "grp")),
        check_vma=False,
    )
```

```python
import functools
import math

import jax
import jax.numpy as jnp
from jax import lax
from jax.experimental import pallas as pl
from jax.experimental.pallas import tpu as pltpu
from jax.sharding import PartitionSpec as P

MESH = pl.DeviceIdType.MESH
LEARN_RATE = 0.3
EPSILON = 1e-06
F32 = jnp.float32
BF16 = jnp.bfloat16


def each(count, body):
    if count <= 64:
        for i in range(count):
            body(i)
    else:

        def step(i, carry):
            body(i)
            return carry

        lax.fori_loop(0, count, step, 0)


def iota(shape, dim):
    return lax.broadcasted_iota(jnp.int32, shape, dim)


def kernel(
    groups,
    lanes,
    place_base,
    accum_base,
    grad_hbm,
    len_hbm,
    look_hbm,
    slot_hbm,
    accum_hbm,
    packed,
    grad_in,
    grad_f32,
    grad_t,
    len_v,
    marks,
    marks_in,
    marks_out,
    slot_v,
    accum_v,
    part,
    recv,
    incoming,
    norm_out,
    norm_in,
    load_sem,
    look_sem,
    a_send,
    a_recv,
    b_send,
    b_recv,
    c_send,
    c_recv,
    near_ready,
    far_ready,
    shadow_in,
    shadow_slot,
    d_send,
    d_recv,
    e_send,
    e_recv,
):
    devices = groups * lanes
    per_peer, embed = recv.shape[1], recv.shape[2]
    slots = groups * per_peer
    tables_all, batch = grad_t.shape[0], grad_t.shape[1]
    tables = tables_all // lanes
    depth = marks.shape[2]
    rows = accum_v.shape[1]
    grp = lax.axis_index("grp")
    lane = lax.axis_index("lane")
    me = grp * lanes + lane
    sign = 2 * (grp // (groups // 2)) - 1

    lane_steps = [(dx, dc) for dx in range(lanes // 2) for dc in range(2)]

    def lane_peer(step, sign):
        dx, dc = step
        half = lanes // 2
        chip = (lane // 2 + sign * dx + half) % half
        return chip * 2 + (lane % 2 + dc) % 2

    def partial_of(m):
        highs, lows = [], []
        for t in range(tables):
            mark = marks[m, t].astype(F32)
            count = jnp.zeros((slots, batch), F32)
            for j in range(depth):
                count += jnp.where(mark[j : j + 1, :] == number, 1.0, 0.0)
            length = len_v[pl.ds(m * tables + t, 1), :].astype(F32)
            factor = count / length
            high = factor.astype(BF16)
            highs.append(high)
            lows.append((factor - high.astype(F32)).astype(BF16))
        factors = jnp.concatenate(
            [jnp.concatenate(highs, axis=1), jnp.concatenate(lows, axis=1)], axis=0
        )
        values = grad_t[pl.ds(m * tables, tables)].reshape(tables * batch, embed)
        both = jnp.dot(factors, values, preferred_element_type=F32)
        return both[:slots] + both[slots:]

    span = groups // 4
    near = groups - span
    is_far = grp >= near
    is_shadow = (grp >= near - span) & (grp < near)

    barrier = pltpu.get_barrier_semaphore()
    peers = [lane_peer(step, 1) for step in lane_steps]

    def signal(semaphore, g, q):
        pl.semaphore_signal(semaphore, inc=1, device_id=(g, q), device_id_type=MESH)

    look_copies = []
    for k, q in enumerate(peers):
        src = look_hbm.at[:, :, pl.ds(pl.multiple_of(q * batch, batch), batch)]
        look_copies.append(pltpu.make_async_copy(src, marks_in.at[k], look_sem.at[k]))
        look_copies[-1].start()
    grad_copy = pltpu.make_async_copy(grad_hbm, grad_in, load_sem.at[0])
    grad_copy.start()
    small_copies = [
        pltpu.make_async_copy(len_hbm, len_v, load_sem.at[1]),
        pltpu.make_async_copy(slot_hbm, slot_v, load_sem.at[2]),
        pltpu.make_async_copy(accum_hbm, accum_v, load_sem.at[3]),
    ]
    for copy in small_copies:
        copy.start()

    with jax.named_scope("signal_up"):
        for q in peers[1:]:
            signal(barrier, grp, q)

        @pl.loop(grp + 1, groups)
        def _(g):
            signal(barrier, g, lane)

    with jax.named_scope("barrier"):
        pl.semaphore_wait(barrier, lanes - 1 + grp)
    with jax.named_scope("signal_down"):

        @pl.when(is_far)
        def _():
            @pl.loop(0, grp)
            def _(g):
                signal(far_ready, g, lane)

        @pl.when(grp < near)
        def _():
            @pl.loop(0, grp)
            def _(g):
                signal(near_ready, g, lane)

    with jax.named_scope("look_wait"):
        for copy in look_copies:
            copy.wait()
    for k in range(1, lanes):
        marks_out[k - 1] = marks_in[k].astype(F32).astype(marks_out.dtype)
    a_copies = []
    for k, q in enumerate(peers[1:], 1):
        copy = pltpu.make_async_remote_copy(
            src_ref=marks_out.at[k - 1],
            dst_ref=marks.at[lane],
            send_sem=a_send.at[k - 1],
            recv_sem=a_recv.at[k - 1],
            device_id=(grp, q),
            device_id_type=MESH,
        )
        copy.start()
        a_copies.append(copy)

    with jax.named_scope("grad_wait"):
        grad_copy.wait()
    with jax.named_scope("grad_turn"):
        for c in range(embed // 128):
            grad_f32[c] = grad_in[:, c * 128 : (c + 1) * 128].astype(F32)
        for t in range(tables_all):
            for c in range(embed // 128):
                grad_t[t, :, c * 128 : (c + 1) * 128] = grad_f32[
                    c, pl.ds(t, batch, stride=tables_all), :
                ].astype(BF16)
    for copy in small_copies:
        copy.wait()
    slot_copy = pltpu.make_async_remote_copy(
        src_ref=slot_v,
        dst_ref=shadow_slot,
        send_sem=e_send,
        recv_sem=e_recv,
        device_id=(jnp.maximum(grp - span, 0), lane),
        device_id_type=MESH,
    )

    @pl.when(is_far)
    def _():
        slot_copy.start()

    marks[lane] = marks_in[0].astype(F32).astype(marks.dtype)
    number = iota((slots, batch), 0).astype(F32)

    for k, step in enumerate(lane_steps):
        m = lane_peer(step, -1)
        if k > 0:
            with jax.named_scope(f"marks_wait{k}"):
                a_copies[k - 1].wait_recv()
        total = partial_of(m)
        for p in range(groups):
            part[m, p] = total[p * per_peer : (p + 1) * per_peer].astype(BF16)

    def send(p, m):
        pltpu.make_async_remote_copy(
            src_ref=part.at[m, p],
            dst_ref=recv.at[me],
            send_sem=b_send,
            recv_sem=b_recv,
            device_id=(p, m),
            device_id_type=MESH,
        ).start()

    def send_shadow(p, m):
        pltpu.make_async_remote_copy(
            src_ref=part.at[m, p],
            dst_ref=shadow_in.at[me],
            send_sem=d_send,
            recv_sem=d_recv,
            device_id=(p - span, m),
            device_id_type=MESH,
        ).start()

    with jax.named_scope("near_wait"):

        @pl.when(grp < near - 1)
        def _():
            pl.semaphore_wait(near_ready, near - 1 - grp)

    with jax.named_scope("near_send"):

        @pl.loop(near, groups)
        def _(p):
            for q in peers[1:]:
                send_shadow(p, q)

            @pl.when(p - span != grp)
            def _():
                send_shadow(p, lane)

            @pl.when(p - span == grp)
            def _():
                pltpu.make_async_copy(part.at[lane, p], shadow_in.at[me], d_recv).start()

        @pl.loop(0, near)
        def _(i):
            p = jnp.where(sign > 0, i, near - 1 - i)

            @pl.when(p != grp)
            def _():
                for m in range(lanes):
                    send(p, m)

        for q in peers[1:]:
            send(grp, q)
        pltpu.make_async_copy(part.at[lane, grp], recv.at[me], b_recv).start()

    with jax.named_scope("far_wait"):

        @pl.when(grp < near)
        def _():
            pl.semaphore_wait(far_ready, span)

        @pl.when(is_far & (grp < groups - 1))
        def _():
            pl.semaphore_wait(far_ready, groups - 1 - grp)

    with jax.named_scope("far_send"):

        @pl.loop(near, groups)
        def _(p):
            @pl.when(p != grp)
            def _():
                for m in range(lanes):
                    send(p, m)

    which = iota((slots, groups), 0)

    def named_rows(slot_ref):
        slot_f = slot_ref[...].astype(F32)
        pick = jnp.zeros((slots, groups), F32)
        for k in range(per_peer):
            pick = jnp.where(which % per_peer == k, slot_f[k : k + 1, :], pick)
        pick = jnp.where(which // per_peer == iota((slots, groups), 1), pick, 0.0)
        return jnp.sum(pick, axis=1, keepdims=True)

    @pl.when(is_shadow)
    def _():
        slot_copy.wait_recv()

    @pl.when(jnp.logical_not(is_shadow))
    def _():
        shadow_slot[...] = jnp.zeros(shadow_slot.shape, jnp.int32)

    incoming[slots:, :] = jnp.zeros((slots, embed), F32)
    own_col = named_rows(slot_v)
    target_col = jnp.concatenate([own_col, named_rows(shadow_slot) + tables * rows], axis=0)
    i_id, j_id = iota((2 * slots, 2 * slots), 0), iota((2 * slots, 2 * slots), 1)
    target_row = jnp.sum(jnp.where(i_id == j_id, target_col, 0.0), axis=0, keepdims=True)
    same = target_col == target_row
    first_col = jnp.sum(jnp.where(same & (j_id < i_id), 1.0, 0.0), axis=1, keepdims=True) == 0.0
    first_row = jnp.sum(jnp.where(same & (i_id < j_id), 1.0, 0.0), axis=0, keepdims=True) == 0.0
    place_row = jnp.where(first_row, target_row, -1.0)
    packed[place_base : place_base + 1, :slots] = place_row[:, :slots]
    same_w = jnp.where(same, 1.0, 0.0).astype(BF16)

    hits = []
    accum_col = jnp.zeros((slots, 1), F32)
    for t in range(tables):
        hit = own_col == (iota((slots, rows), 1) + t * rows).astype(F32)
        hits.append(hit)
        accum_col += jnp.sum(
            jnp.where(hit, accum_v[t : t + 1, :], 0.0), axis=1, keepdims=True
        )

    def gather(source, base):
        for g in range(groups):
            group_sum = source[g * lanes].astype(F32)
            for q in range(1, lanes):
                group_sum += source[g * lanes + q].astype(F32)
            incoming[base + g * per_peer : base + (g + 1) * per_peer, :] = group_sum

    @pl.when(is_shadow)
    def _():
        with jax.named_scope("shadow_wait"):
            pltpu.make_async_copy(shadow_in, shadow_in, d_recv).wait()
        gather(shadow_in, slots)

    with jax.named_scope("sums_wait"):
        pltpu.make_async_copy(recv, recv, b_recv).wait()
    gather(recv, 0)
    all_grads = jnp.dot(same_w, incoming[...].astype(BF16), preferred_element_type=F32)
    square_all = jnp.sum(all_grads * all_grads, axis=1, keepdims=True) * (1.0 / embed)
    square_first = jnp.where(first_col, square_all, 0.0)
    local = embed * jnp.sum(square_first, axis=0, keepdims=True)
    norm_out[...] = jnp.broadcast_to(local, (1, 128))
    grads, square_col = all_grads[:slots], square_all[:slots]

    def tell(far):
        pltpu.make_async_remote_copy(
            src_ref=norm_out,
            dst_ref=norm_in.at[me],
            send_sem=c_send,
            recv_sem=c_recv,
            device_id=(far // lanes, far % lanes),
            device_id_type=MESH,
        ).start()

    @pl.when(jnp.logical_not(is_far))
    def _():
        if devices <= 64:
            for d in range(1, devices):
                tell((me + sign * d + devices) % devices)
        else:
            each(devices - 1, lambda i: tell((me + i + 1) % devices))
        pltpu.make_async_copy(norm_out, norm_in.at[me], c_recv).start()

    square_rows = [
        jnp.sum(jnp.where(hit, square_first[:slots], 0.0), axis=0, keepdims=True) for hit in hits
    ]
    for copy in a_copies:
        copy.wait_send()
    sent = recv.at[pl.ds(0, devices - 1)]
    pltpu.make_async_copy(sent, sent, b_send).wait()

    def sent_shadows(count):
        sent = shadow_in.at[pl.ds(0, count)]
        pltpu.make_async_copy(sent, sent, d_send).wait()

    if span > 0:
        pl.when(is_shadow)(lambda: sent_shadows(span * lanes - 1))
        pl.when(jnp.logical_not(is_shadow))(lambda: sent_shadows(span * lanes))

    @pl.when(is_far)
    def _():
        slot_copy.wait_send()

    with jax.named_scope("norm_wait"):
        told = norm_in.at[pl.ds(0, near * lanes)]
        pltpu.make_async_copy(told, told, c_recv).wait()
    norm_total = jnp.sum(norm_in[: near * lanes], axis=0)[:, :1]
    clip_limit = 0.5 * math.sqrt(devices * slots * embed)
    clip = clip_limit / jnp.maximum(jnp.sqrt(norm_total), clip_limit)
    for t in range(tables):
        packed[accum_base + t : accum_base + t + 1, :rows] = accum_v[t : t + 1, :] + clip * clip * square_rows[t]
    new_accum_col = accum_col + clip * clip * square_col
    delta = LEARN_RATE * clip * grads / (jnp.sqrt(new_accum_col) + EPSILON)
    packed[:slots, :embed] = delta

    @pl.when(jnp.logical_not(is_far))
    def _():
        told = norm_in.at[pl.ds(0, devices - 1)]
        pltpu.make_async_copy(told, told, c_send).wait()


def update_kernel(
    chunk, slots, place_base, accum_base, weights, packed, wout, aout, held, accum, sems, accum_sem
):
    accum[...] = packed[accum_base : accum_base + accum.shape[0], : accum.shape[1]]
    accum_copy = pltpu.make_async_copy(accum, aout, accum_sem)
    accum_copy.start()
    delta = packed[:slots, : weights.shape[2]]
    high = delta.astype(BF16)
    deltas = jnp.concatenate([high, (delta - high.astype(F32)).astype(BF16)], axis=0)
    place_row = packed[place_base : place_base + 1, :slots]
    place_row = jnp.concatenate([place_row, place_row], axis=1)
    tables, rows = weights.shape[0], weights.shape[1]
    copies = []
    for t in range(tables):
        for c in range(0, rows, chunk):
            row_id = (iota((chunk, 1), 0) + (t * rows + c)).astype(F32)
            place = jnp.where(row_id == place_row, 1.0, 0.0).astype(BF16)
            held[t, c : c + chunk] = weights[t, c : c + chunk] - jnp.dot(
                place, deltas, preferred_element_type=F32
            )
            copies.append(
                pltpu.make_async_copy(
                    held.at[t, pl.ds(c, chunk)],
                    wout.at[t, pl.ds(c, chunk)],
                    sems.at[len(copies)],
                )
            )
            copies[-1].start()
    for copy in copies:
        copy.wait()
    accum_copy.wait()


def per_device(groups, lanes, grad_pooled, bag_len, lookup_slot, slot_row, weights, accum):
    batch, tables_all, embed = grad_pooled.shape
    samples, tables, depth = lookup_slot.shape
    rows = accum.shape[1]
    per_peer = slot_row.shape[3]
    devices = groups * lanes
    slots = groups * per_peer
    mark_type = BF16 if slots <= 256 else F32
    place_base = -(-slots // 8) * 8
    accum_base = place_base + 8
    packed_shape = (accum_base + -(-tables // 8) * 8, max(embed, rows, slots))
    anywhere = pl.BlockSpec(memory_space=pl.ANY)
    vmem = pl.BlockSpec(memory_space=pltpu.VMEM)
    packed = pl.pallas_call(
        functools.partial(kernel, groups, lanes, place_base, accum_base),
        out_shape=jax.ShapeDtypeStruct(packed_shape, F32),
        in_specs=[pl.BlockSpec(memory_space=pltpu.HBM)] * 5,
        out_specs=vmem,
        cost_estimate=pl.CostEstimate(
            flops=8 * slots * batch * tables_all * embed,
            bytes_accessed=32 * batch * tables_all * embed,
            transcendentals=0,
        ),
        scratch_shapes=[
            pltpu.VMEM((batch * tables_all, embed), BF16),
            pltpu.VMEM((embed // 128, batch * tables_all, 128), F32),
            pltpu.VMEM((tables_all, batch, embed), BF16),
            pltpu.VMEM((tables_all, batch), jnp.int32),
            pltpu.VMEM((lanes, tables, depth, batch), mark_type),
            pltpu.VMEM((lanes, tables, depth, batch), jnp.int32),
            pltpu.VMEM((lanes - 1, tables, depth, batch), mark_type),
            pltpu.VMEM((per_peer, groups), jnp.int32),
            pltpu.VMEM((tables, rows), F32),
            pltpu.VMEM((lanes, groups, per_peer, embed), BF16),
            pltpu.VMEM((devices, per_peer, embed), BF16),
            pltpu.VMEM((2 * slots, embed), F32),
            pltpu.VMEM((1, 128), F32),
            pltpu.VMEM((devices, 1, 128), F32),
            pltpu.SemaphoreType.DMA((4,)),
            pltpu.SemaphoreType.DMA((lanes,)),
            pltpu.SemaphoreType.DMA((lanes - 1,)),
            pltpu.SemaphoreType.DMA((lanes - 1,)),
            pltpu.SemaphoreType.DMA,
            pltpu.SemaphoreType.DMA,
            pltpu.SemaphoreType.DMA,
            pltpu.SemaphoreType.DMA,
            pltpu.SemaphoreType.REGULAR,
            pltpu.SemaphoreType.REGULAR,
            pltpu.VMEM((devices, per_peer, embed), BF16),
            pltpu.VMEM((per_peer, groups), jnp.int32),
            pltpu.SemaphoreType.DMA,
            pltpu.SemaphoreType.DMA,
            pltpu.SemaphoreType.DMA,
            pltpu.SemaphoreType.DMA,
        ],
        compiler_params=pltpu.CompilerParams(
            collective_id=0, has_side_effects=True, vmem_limit_bytes=32 << 20
        ),
    )(
        *(
            pltpu.with_memory_space_constraint(operand, pltpu.HBM)
            for operand in (
                grad_pooled.reshape(batch * tables_all, embed),
                bag_len.T,
                jnp.transpose(lookup_slot, (1, 2, 0)),
                slot_row.reshape(groups, per_peer).T,
                accum,
            )
        )
    )
    chunk = min(rows, 128)
    return pl.pallas_call(
        functools.partial(update_kernel, chunk, slots, place_base, accum_base),
        out_shape=(
            jax.ShapeDtypeStruct(weights.shape, F32),
            jax.ShapeDtypeStruct(accum.shape, F32),
        ),
        in_specs=[vmem, vmem],
        out_specs=(anywhere, anywhere),
        scratch_shapes=[
            pltpu.VMEM(weights.shape, F32),
            pltpu.VMEM(accum.shape, F32),
            pltpu.SemaphoreType.DMA((tables * (rows // chunk),)),
            pltpu.SemaphoreType.DMA,
        ],
        compiler_params=pltpu.CompilerParams(vmem_limit_bytes=8 << 20),
    )(weights, packed)


def solution(mesh):
    placed = (
        P(("grp", "lane"), None, None),
        P(("grp", "lane"), None),
        P("grp", "lane", None),
        P("grp", "lane", None, None),
        P("lane", "grp", None),
        P("lane", "grp"),
    )
    return jax.shard_map(
        functools.partial(per_device, mesh.shape["grp"], mesh.shape["lane"]),
        mesh=mesh,
        in_specs=placed,
        out_specs=(P("lane", "grp", None), P("lane", "grp")),
        check_vma=False,
    )
```

```python
import functools
import math

import jax
import jax.numpy as jnp
from jax import lax
from jax.experimental import pallas as pl
from jax.experimental.pallas import tpu as pltpu
from jax.sharding import PartitionSpec as P

MESH = pl.DeviceIdType.MESH
LEARN_RATE = 0.3
EPSILON = 1e-06
F32 = jnp.float32
BF16 = jnp.bfloat16


def each(count, body):
    if count <= 64:
        for i in range(count):
            body(i)
    else:

        def step(i, carry):
            body(i)
            return carry

        lax.fori_loop(0, count, step, 0)


def iota(shape, dim):
    return lax.broadcasted_iota(jnp.int32, shape, dim)


def kernel(
    groups,
    lanes,
    place_base,
    accum_base,
    grad_hbm,
    len_hbm,
    look_hbm,
    slot_hbm,
    accum_hbm,
    weights_hbm,
    packed,
    held,
    grad_in,
    grad_f32,
    grad_t,
    len_v,
    marks,
    marks_in,
    marks_out,
    slot_v,
    accum_v,
    part_f,
    part,
    recv,
    sums,
    shadow_sums,
    norm_out,
    norm_in,
    load_sem,
    look_sem,
    a_send,
    a_recv,
    b_send,
    b_recv,
    c_send,
    c_recv,
    near_ready,
    far_ready,
    shadow_in,
    pair_slot,
    shadow_slot,
    d_send,
    d_recv,
    e_send,
    e_recv,
    f_send,
    f_recv,
    g_send,
    g_recv,
):
    devices = groups * lanes
    per_peer, embed = slot_v.shape[0], grad_t.shape[2]
    slots = groups * per_peer
    tables_all, batch = grad_t.shape[0], grad_t.shape[1]
    tables = tables_all // lanes
    depth = marks.shape[2]
    rows = accum_v.shape[1]
    grp = lax.axis_index("grp")
    lane = lax.axis_index("lane")
    me = grp * lanes + lane
    sign = 2 * (grp // (groups // 2)) - 1

    lane_steps = [(dx, dc) for dx in range(lanes // 2) for dc in range(2)]

    def lane_peer(step, sign):
        dx, dc = step
        half = lanes // 2
        chip = (lane // 2 + sign * dx + half) % half
        return chip * 2 + (lane % 2 + dc) % 2

    def partial_of(m):
        highs, lows = [], []
        for t in range(tables):
            mark = marks[m, t].astype(F32)
            count = jnp.zeros((slots, batch), F32)
            for j in range(depth):
                count += jnp.where(mark[j : j + 1, :] == number, 1.0, 0.0)
            length = len_v[pl.ds(m * tables + t, 1), :].astype(F32)
            factor = count / length
            high = factor.astype(BF16)
            highs.append(high)
            lows.append((factor - high.astype(F32)).astype(BF16))
        factors = jnp.concatenate(
            [jnp.concatenate(highs, axis=1), jnp.concatenate(lows, axis=1)], axis=0
        )
        values = grad_t[pl.ds(m * tables, tables)].reshape(tables * batch, embed)
        both = jnp.dot(factors, values, preferred_element_type=F32)
        return both[:slots] + both[slots:]

    span = groups // 4
    near = groups - span
    half = lanes // 2
    column, core = lane // 2, lane % 2
    leader = core == 1
    widths = embed // 128
    tile = recv.shape[1]
    is_far = grp >= near
    tells = leader & (grp < near)
    is_shadow = leader & (grp >= near - span) & (grp < near)

    barrier = pltpu.get_barrier_semaphore()
    peers = [lane_peer(step, 1) for step in lane_steps]

    def signal(semaphore, g, q):
        pl.semaphore_signal(semaphore, inc=1, device_id=(g, q), device_id_type=MESH)

    look_copies = []
    for k, q in enumerate(peers):
        src = look_hbm.at[:, :, pl.ds(pl.multiple_of(q * batch, batch), batch)]
        look_copies.append(pltpu.make_async_copy(src, marks_in.at[k], look_sem.at[k]))
        look_copies[-1].start()
    grad_copy = pltpu.make_async_copy(grad_hbm, grad_in, load_sem.at[0])
    weights_copy = pltpu.make_async_copy(weights_hbm, held, load_sem.at[4])
    small_copies = [
        pltpu.make_async_copy(len_hbm, len_v, load_sem.at[1]),
        pltpu.make_async_copy(slot_hbm, slot_v, load_sem.at[2]),
        pltpu.make_async_copy(accum_hbm, accum_v, load_sem.at[3]),
    ]

    with jax.named_scope("signal_up"):
        for q in peers[1:]:
            signal(barrier, grp, q)

        @pl.loop(grp + 1, groups)
        def _(g):
            signal(barrier, g, lane)

    grad_copy.start()
    for copy in small_copies:
        copy.start()

    with jax.named_scope("barrier"):
        pl.semaphore_wait(barrier, lanes - 1 + grp)
    with jax.named_scope("signal_down"):

        @pl.when(is_far)
        def _():
            @pl.loop(0, grp)
            def _(g):
                signal(far_ready, g, lane)

        @pl.when(grp < near)
        def _():
            @pl.loop(0, grp)
            def _(g):
                signal(near_ready, g, lane)

    with jax.named_scope("look_wait"):
        for copy in look_copies:
            copy.wait()
    for k in range(1, lanes):
        marks_out[k - 1] = marks_in[k].astype(F32).astype(marks_out.dtype)
    a_copies = []
    for k, q in enumerate(peers[1:], 1):
        copy = pltpu.make_async_remote_copy(
            src_ref=marks_out.at[k - 1],
            dst_ref=marks.at[lane],
            send_sem=a_send.at[k - 1],
            recv_sem=a_recv.at[k - 1],
            device_id=(grp, q),
            device_id_type=MESH,
        )
        copy.start()
        a_copies.append(copy)

    with jax.named_scope("grad_wait"):
        grad_copy.wait()
    weights_copy.start()
    with jax.named_scope("grad_turn"):
        for c in range(embed // 128):
            grad_f32[c] = grad_in[:, c * 128 : (c + 1) * 128].astype(F32)
        for t in range(tables_all):
            for c in range(embed // 128):
                grad_t[t, :, c * 128 : (c + 1) * 128] = grad_f32[
                    c, pl.ds(t, batch, stride=tables_all), :
                ].astype(BF16)
    for copy in small_copies:
        copy.wait()
    pair_copy = pltpu.make_async_remote_copy(
        src_ref=slot_v,
        dst_ref=pair_slot,
        send_sem=e_send,
        recv_sem=e_recv,
        device_id=(grp, lane - core + 1),
        device_id_type=MESH,
    )
    slot_copy = pltpu.make_async_remote_copy(
        src_ref=slot_v,
        dst_ref=shadow_slot.at[core],
        send_sem=f_send,
        recv_sem=f_recv,
        device_id=(jnp.maximum(grp - span, 0), lane - core + 1),
        device_id_type=MESH,
    )

    @pl.when(core == 0)
    def _():
        pair_copy.start()
        pair_slot[...] = jnp.zeros(pair_slot.shape, jnp.int32)

    @pl.when(jnp.logical_not(is_shadow))
    def _():
        shadow_slot[...] = jnp.zeros(shadow_slot.shape, jnp.int32)

    shadow_sums[...] = jnp.zeros(shadow_sums.shape, BF16)

    marks[lane] = marks_in[0].astype(F32).astype(marks.dtype)
    number = iota((slots, batch), 0).astype(F32)

    for k, step in enumerate(lane_steps):
        m = lane_peer(step, -1)
        if k > 0:
            with jax.named_scope(f"marks_wait{k}"):
                a_copies[k - 1].wait_recv()
        if k == 1:

            @pl.when(is_far)
            def _():
                slot_copy.start()

        total = partial_of(m)
        for h in range(widths):
            part_f[m // 2, pl.ds(m % 2 * widths + h, slots, stride=2 * widths), :] = total[
                :, h * 128 : (h + 1) * 128
            ]
    for x in range(half):
        for p in range(groups):
            part[x, p] = part_f[x, p * tile : (p + 1) * tile].astype(BF16)

    def send(p, x):
        pltpu.make_async_remote_copy(
            src_ref=part.at[x, p],
            dst_ref=recv.at[me],
            send_sem=b_send,
            recv_sem=b_recv,
            device_id=(p, 2 * x + 1),
            device_id_type=MESH,
        ).start()

    def send_shadow(p, x):
        pltpu.make_async_remote_copy(
            src_ref=part.at[x, p],
            dst_ref=shadow_in.at[me],
            send_sem=d_send,
            recv_sem=d_recv,
            device_id=(p - span, 2 * x + 1),
            device_id_type=MESH,
        ).start()

    def mine(p, x):
        return leader & (p == grp) & (x == column)

    with jax.named_scope("near_wait"):

        @pl.when(grp < near - 1)
        def _():
            pl.semaphore_wait(near_ready, near - 1 - grp)

    with jax.named_scope("near_send"):

        @pl.loop(near, groups)
        def _(p):
            for x in range(half):
                here = mine(p - span, x)

                @pl.when(jnp.logical_not(here))
                def _():
                    send_shadow(p, x)

                @pl.when(here)
                def _():
                    pltpu.make_async_copy(part.at[x, p], shadow_in.at[me], d_recv).start()

        @pl.loop(0, near)
        def _(i):
            p = jnp.where(sign > 0, i, near - 1 - i)
            for x in range(half):

                @pl.when(jnp.logical_not(mine(p, x)))
                def _():
                    send(p, x)

        @pl.when(leader)
        def _():
            pltpu.make_async_copy(part.at[column, grp], recv.at[me], b_recv).start()

    with jax.named_scope("far_wait"):

        @pl.when(grp < near)
        def _():
            pl.semaphore_wait(far_ready, span)

        @pl.when(is_far & (grp < groups - 1))
        def _():
            pl.semaphore_wait(far_ready, groups - 1 - grp)

    with jax.named_scope("far_send"):

        @pl.loop(near, groups)
        def _(p):
            for x in range(half):

                @pl.when(jnp.logical_not(mine(p, x)))
                def _():
                    send(p, x)

    two = 2 * slots
    which = iota((two, groups), 0)
    span_of = tables * rows

    def named_rows(low, high):
        low, high = low.astype(F32), high.astype(F32)
        pick = jnp.zeros((two, groups), F32)
        for k in range(per_peer):
            pick = jnp.where(which % (2 * per_peer) == 2 * k, low[k : k + 1, :], pick)
            pick = jnp.where(which % (2 * per_peer) == 2 * k + 1, high[k : k + 1, :], pick)
        pick = jnp.where(which // (2 * per_peer) == iota((two, groups), 1), pick, 0.0)
        return jnp.sum(pick, axis=1, keepdims=True)

    @pl.when(leader)
    def _():
        pair_copy.wait_recv()

    @pl.when(is_shadow)
    def _():
        pltpu.make_async_copy(shadow_slot, shadow_slot, f_recv).wait()

    own_slot, other_slot = slot_v[...], pair_slot[...] + span_of
    target_col = jnp.concatenate(
        [
            named_rows(
                jnp.where(leader, other_slot, own_slot), jnp.where(leader, own_slot, other_slot)
            ),
            named_rows(shadow_slot[0] + 2 * span_of, shadow_slot[1] + 3 * span_of),
        ],
        axis=0,
    )
    i_id, j_id = iota((2 * two, 2 * two), 0), iota((2 * two, 2 * two), 1)
    target_row = jnp.sum(jnp.where(i_id == j_id, target_col, 0.0), axis=0, keepdims=True)
    same = target_col == target_row
    first_col = jnp.sum(jnp.where(same & (j_id < i_id), 1.0, 0.0), axis=1, keepdims=True) == 0.0
    first_row = jnp.sum(jnp.where(same & (i_id < j_id), 1.0, 0.0), axis=0, keepdims=True) == 0.0
    is_own = (target_row < span_of) & first_row
    place_row = jnp.where(is_own, target_row, -1.0)
    packed[place_base : place_base + 1, :two] = place_row[:, :two]
    wide = (2 * two, widths * 2 * two)
    wide_i, wide_j = iota(wide, 0), iota(wide, 1)
    spread_row = jnp.sum(
        jnp.where(wide_i == wide_j // widths, target_col, 0.0), axis=0, keepdims=True
    )
    picks = [
        jnp.where((target_col == spread_row) & (wide_j % widths == h), 1.0, 0.0).astype(BF16)
        for h in range(widths)
    ]

    hits = []
    accum_col = jnp.zeros((two, 1), F32)
    for t in range(tables):
        hit = target_col[:two] == (iota((two, rows), 1) + t * rows).astype(F32)
        hits.append(hit)
        accum_col += jnp.sum(
            jnp.where(hit, accum_v[t : t + 1, :], 0.0), axis=1, keepdims=True
        )

    def gather(source):
        group_sums = []
        for g in range(groups):
            group_sum = source[g * lanes].astype(F32)
            for q in range(1, lanes):
                group_sum += source[g * lanes + q].astype(F32)
            group_sums.append(group_sum)
        return jnp.concatenate(group_sums, axis=0).astype(BF16)

    sums_copy = pltpu.make_async_remote_copy(
        src_ref=sums,
        dst_ref=sums,
        send_sem=g_send,
        recv_sem=g_recv,
        device_id=(grp, lane - core),
        device_id_type=MESH,
    )

    @pl.when(is_shadow)
    def _():
        with jax.named_scope("shadow_wait"):
            pltpu.make_async_copy(shadow_in, shadow_in, d_recv).wait()
        shadow_sums[...] = gather(shadow_in)

    with jax.named_scope("sums_wait"):

        @pl.when(leader)
        def _():
            pltpu.make_async_copy(recv, recv, b_recv).wait()
            sums[...] = gather(recv)
            sums_copy.start()

        @pl.when(core == 0)
        def _():
            sums_copy.wait_recv()

    all_sums = jnp.concatenate([sums[...], shadow_sums[...]], axis=0)
    pieces = [jnp.dot(pick, all_sums, preferred_element_type=F32) for pick in picks]
    square_all = sum(piece * piece for piece in pieces)
    square_all = jnp.sum(square_all, axis=1, keepdims=True) * (1.0 / embed)
    square_first = jnp.where(first_col, square_all, 0.0)
    local = embed * jnp.sum(square_first, axis=0, keepdims=True)
    grads = jnp.concatenate([piece[:two] for piece in pieces], axis=1)
    square_col = square_all[:two]
    norm_out[...] = jnp.broadcast_to(local, (1, 128))

    def tell(far):
        pltpu.make_async_remote_copy(
            src_ref=norm_out,
            dst_ref=norm_in.at[grp * half + column],
            send_sem=c_send,
            recv_sem=c_recv,
            device_id=(far // lanes, far % lanes),
            device_id_type=MESH,
        ).start()

    @pl.when(tells)
    def _():
        if devices <= 64:
            for d in range(1, devices):
                tell((me + sign * d + devices) % devices)
        else:
            each(devices - 1, lambda i: tell((me + i + 1) % devices))
        pltpu.make_async_copy(norm_out, norm_in.at[grp * half + column], c_recv).start()

    square_rows = [
        jnp.sum(jnp.where(hit, square_first[:two], 0.0), axis=0, keepdims=True) for hit in hits
    ]
    for copy in a_copies:
        copy.wait_send()

    def sent(buffer, count, semaphore):
        piece = buffer.at[pl.ds(0, count)]
        pltpu.make_async_copy(piece, piece, semaphore).wait()

    pl.when(leader)(lambda: sent(recv, groups * half - 1, b_send))
    pl.when(core == 0)(lambda: sent(recv, groups * half, b_send))
    if span > 0:
        pl.when(is_shadow)(lambda: sent(shadow_in, span * half - 1, d_send))
        pl.when(jnp.logical_not(is_shadow))(lambda: sent(shadow_in, span * half, d_send))

    @pl.when(is_far)
    def _():
        slot_copy.wait_send()

    @pl.when(core == 0)
    def _():
        pair_copy.wait_send()

    @pl.when(leader)
    def _():
        sums_copy.wait_send()

    with jax.named_scope("norm_wait"):
        told = norm_in.at[pl.ds(0, near * half)]
        pltpu.make_async_copy(told, told, c_recv).wait()
    weights_copy.wait()
    norm_total = jnp.sum(norm_in[: near * half], axis=0)[:, :1]
    clip_limit = 0.5 * math.sqrt(devices * slots * embed)
    clip = clip_limit / jnp.maximum(jnp.sqrt(norm_total), clip_limit)
    for t in range(tables):
        packed[accum_base + t : accum_base + t + 1, :rows] = accum_v[t : t + 1, :] + clip * clip * square_rows[t]
    new_accum_col = accum_col + clip * clip * square_col
    delta = LEARN_RATE * clip * grads / (jnp.sqrt(new_accum_col) + EPSILON)
    packed[:two, :embed] = delta

    @pl.when(tells)
    def _():
        told = norm_in.at[pl.ds(0, devices - 1)]
        pltpu.make_async_copy(told, told, c_send).wait()


def update_kernel(
    chunk, slots, place_base, accum_base, weights, packed, wout, aout, held, accum, sems, accum_sem
):
    accum[...] = packed[accum_base : accum_base + accum.shape[0], : accum.shape[1]]
    accum_copy = pltpu.make_async_copy(accum, aout, accum_sem)
    accum_copy.start()
    delta = packed[:slots, : weights.shape[2]]
    high = delta.astype(BF16)
    deltas = jnp.concatenate([high, (delta - high.astype(F32)).astype(BF16)], axis=0)
    place_row = packed[place_base : place_base + 1, :slots]
    place_row = jnp.concatenate([place_row, place_row], axis=1)
    tables, rows = weights.shape[0], weights.shape[1]
    copies = []
    for t in range(tables):
        for c in range(0, rows, chunk):
            row_id = (iota((chunk, 1), 0) + (t * rows + c)).astype(F32)
            place = jnp.where(row_id == place_row, 1.0, 0.0).astype(BF16)
            held[t, c : c + chunk] = weights[t, c : c + chunk] - jnp.dot(
                place, deltas, preferred_element_type=F32
            )
            copies.append(
                pltpu.make_async_copy(
                    held.at[t, pl.ds(c, chunk)],
                    wout.at[t, pl.ds(c, chunk)],
                    sems.at[len(copies)],
                )
            )
            copies[-1].start()
    for copy in copies:
        copy.wait()
    accum_copy.wait()


def per_device(groups, lanes, grad_pooled, bag_len, lookup_slot, slot_row, weights, accum):
    batch, tables_all, embed = grad_pooled.shape
    samples, tables, depth = lookup_slot.shape
    rows = accum.shape[1]
    per_peer = slot_row.shape[3]
    devices = groups * lanes
    slots = groups * per_peer
    mark_type = BF16 if slots <= 256 else F32
    half = lanes // 2
    tile = 2 * per_peer * (embed // 128)
    place_base = -(-2 * slots // 8) * 8
    accum_base = place_base + 8
    packed_shape = (accum_base + -(-tables // 8) * 8, max(embed, rows, 2 * slots))
    anywhere = pl.BlockSpec(memory_space=pl.ANY)
    vmem = pl.BlockSpec(memory_space=pltpu.VMEM)
    packed, held = pl.pallas_call(
        functools.partial(kernel, groups, lanes, place_base, accum_base),
        out_shape=(
            jax.ShapeDtypeStruct(packed_shape, F32),
            jax.ShapeDtypeStruct(weights.shape, F32),
        ),
        in_specs=[pl.BlockSpec(memory_space=pltpu.HBM)] * 6,
        out_specs=(vmem, vmem),
        cost_estimate=pl.CostEstimate(
            flops=8 * slots * batch * tables_all * embed,
            bytes_accessed=32 * batch * tables_all * embed,
            transcendentals=0,
        ),
        scratch_shapes=[
            pltpu.VMEM((batch * tables_all, embed), BF16),
            pltpu.VMEM((embed // 128, batch * tables_all, 128), F32),
            pltpu.VMEM((tables_all, batch, embed), BF16),
            pltpu.VMEM((tables_all, batch), jnp.int32),
            pltpu.VMEM((lanes, tables, depth, batch), mark_type),
            pltpu.VMEM((lanes, tables, depth, batch), jnp.int32),
            pltpu.VMEM((lanes - 1, tables, depth, batch), mark_type),
            pltpu.VMEM((per_peer, groups), jnp.int32),
            pltpu.VMEM((tables, rows), F32),
            pltpu.VMEM((half, groups * tile, 128), F32),
            pltpu.VMEM((half, groups, tile, 128), BF16),
            pltpu.VMEM((devices, tile, 128), BF16),
            pltpu.VMEM((groups * tile, 128), BF16),
            pltpu.VMEM((groups * tile, 128), BF16),
            pltpu.VMEM((1, 128), F32),
            pltpu.VMEM((devices, 1, 128), F32),
            pltpu.SemaphoreType.DMA((5,)),
            pltpu.SemaphoreType.DMA((lanes,)),
            pltpu.SemaphoreType.DMA((lanes - 1,)),
            pltpu.SemaphoreType.DMA((lanes - 1,)),
            pltpu.SemaphoreType.DMA,
            pltpu.SemaphoreType.DMA,
            pltpu.SemaphoreType.DMA,
            pltpu.SemaphoreType.DMA,
            pltpu.SemaphoreType.REGULAR,
            pltpu.SemaphoreType.REGULAR,
            pltpu.VMEM((devices, tile, 128), BF16),
            pltpu.VMEM((per_peer, groups), jnp.int32),
            pltpu.VMEM((2, per_peer, groups), jnp.int32),
            pltpu.SemaphoreType.DMA,
            pltpu.SemaphoreType.DMA,
            pltpu.SemaphoreType.DMA,
            pltpu.SemaphoreType.DMA,
            pltpu.SemaphoreType.DMA,
            pltpu.SemaphoreType.DMA,
            pltpu.SemaphoreType.DMA,
            pltpu.SemaphoreType.DMA,
        ],
        compiler_params=pltpu.CompilerParams(
            collective_id=0, has_side_effects=True, vmem_limit_bytes=32 << 20
        ),
    )(
        *(
            pltpu.with_memory_space_constraint(operand, pltpu.HBM)
            for operand in (
                grad_pooled.reshape(batch * tables_all, embed),
                bag_len.T,
                jnp.transpose(lookup_slot, (1, 2, 0)),
                slot_row.reshape(groups, per_peer).T,
                accum,
                weights,
            )
        )
    )
    chunk = min(rows, 128)
    return pl.pallas_call(
        functools.partial(update_kernel, chunk, 2 * slots, place_base, accum_base),
        out_shape=(
            jax.ShapeDtypeStruct(weights.shape, F32),
            jax.ShapeDtypeStruct(accum.shape, F32),
        ),
        in_specs=[vmem, vmem],
        out_specs=(anywhere, anywhere),
        scratch_shapes=[
            pltpu.VMEM(weights.shape, F32),
            pltpu.VMEM(accum.shape, F32),
            pltpu.SemaphoreType.DMA((tables * (rows // chunk),)),
            pltpu.SemaphoreType.DMA,
        ],
        compiler_params=pltpu.CompilerParams(vmem_limit_bytes=8 << 20),
    )(held, packed)


def solution(mesh):
    placed = (
        P(("grp", "lane"), None, None),
        P(("grp", "lane"), None),
        P("grp", "lane", None),
        P("grp", "lane", None, None),
        P("lane", "grp", None),
        P("lane", "grp"),
    )
    return jax.shard_map(
        functools.partial(per_device, mesh.shape["grp"], mesh.shape["lane"]),
        mesh=mesh,
        in_specs=placed,
        out_specs=(P("lane", "grp", None), P("lane", "grp")),
        check_vma=False,
    )
```

```python
import functools
import math

import jax
import jax.numpy as jnp
from jax import lax
from jax.experimental import pallas as pl
from jax.experimental.pallas import tpu as pltpu
from jax.sharding import PartitionSpec as P

MESH = pl.DeviceIdType.MESH
LEARN_RATE = 0.3
EPSILON = 1e-06
SIDE = 2
F32 = jnp.float32
BF16 = jnp.bfloat16


def each(count, body):
    if count <= 64:
        for i in range(count):
            body(i)
    else:

        def step(i, carry):
            body(i)
            return carry

        lax.fori_loop(0, count, step, 0)


def iota(shape, dim):
    return lax.broadcasted_iota(jnp.int32, shape, dim)


def kernel(
    groups,
    lanes,
    place_base,
    accum_base,
    grad_hbm,
    len_hbm,
    look_hbm,
    slot_hbm,
    accum_hbm,
    weights_hbm,
    packed,
    held,
    grad_in,
    grad_f32,
    grad_t,
    len_v,
    marks,
    marks_in,
    marks_out,
    slot_v,
    accum_v,
    part_f,
    part,
    recv,
    sums,
    shadow_sums,
    norm_out,
    norm_in,
    load_sem,
    look_sem,
    a_send,
    a_recv,
    b_send,
    b_recv,
    c_send,
    c_recv,
    near_ready,
    far_ready,
    top_ready,
    shadow_in,
    pair_slot,
    shadow_slot,
    d_send,
    d_recv,
    e_send,
    e_recv,
    f_send,
    f_recv,
    g_send,
    g_recv,
):
    devices = groups * lanes
    per_peer, embed = slot_v.shape[0], grad_t.shape[2]
    slots = groups * per_peer
    tables_all, batch = grad_t.shape[0], grad_t.shape[1]
    tables = tables_all // lanes
    depth = marks.shape[2]
    rows = accum_v.shape[1]
    grp = lax.axis_index("grp")
    lane = lax.axis_index("lane")
    me = grp * lanes + lane
    sign = 2 * (grp // (groups // 2)) - 1

    def partial_of(m):
        highs, lows = [], []
        for t in range(tables):
            mark = marks[m, t].astype(F32)
            count = jnp.zeros((slots, batch), F32)
            for j in range(depth):
                count += jnp.where(mark[j : j + 1, :] == number, 1.0, 0.0)
            length = len_v[pl.ds(m * tables + t, 1), :].astype(F32)
            factor = count / length
            high = factor.astype(BF16)
            highs.append(high)
            lows.append((factor - high.astype(F32)).astype(BF16))
        factors = jnp.concatenate(
            [jnp.concatenate(highs, axis=1), jnp.concatenate(lows, axis=1)], axis=0
        )
        values = grad_t[pl.ds(m * tables, tables)].reshape(tables * batch, embed)
        both = jnp.dot(factors, values, preferred_element_type=F32)
        return both[:slots] + both[slots:]

    side = SIDE if groups % (4 * SIDE) == 0 else 1
    depth_all = groups // side
    span = depth_all // 4 * side
    near = groups - span
    near_depth = near // side
    far_depth = depth_all - near_depth
    row, place = grp // side, grp % side
    rows_above, places_above = depth_all - row, side - place
    near_above = jnp.maximum(near_depth - row, 0) * places_above - jnp.where(grp < near, 1, 0)
    far_above = jnp.minimum(rows_above, far_depth) * places_above - jnp.where(grp < near, 0, 1)

    def is_apart(g):
        r, p = g // side, g % side
        return ((r > 0) & (p < side - 1)) | ((r < depth_all - 1) & (p > 0))


    def above(g):
        return (g // side >= row) & (g % side >= place) & (g != grp)

    def below(g):
        return (g // side <= row) & (g % side <= place) & (g != grp)

    half = lanes // 2
    column, core = lane // 2, lane % 2
    leader = core == 1
    widths = embed // 128
    tile = recv.shape[1]
    is_far = grp >= near
    is_top = leader & (grp == groups - 1)
    tells = leader & (grp < near)
    is_shadow = leader & (grp >= near - span) & (grp < near)

    barrier = pltpu.get_barrier_semaphore()
    partner = lane + 1 - 2 * core
    others = [lax.rem(column + d, half) for d in range(1, half)]
    peers = [lane] + [2 * x for x in others] + [2 * x + 1 for x in others] + [partner]

    def signal(semaphore, g, q):
        pl.semaphore_signal(semaphore, inc=1, device_id=(g, q), device_id_type=MESH)

    look_copies = []
    for k, q in enumerate(peers):
        src = look_hbm.at[:, :, pl.ds(pl.multiple_of(q * batch, batch), batch)]
        look_copies.append(pltpu.make_async_copy(src, marks_in.at[k], look_sem.at[k]))
        look_copies[-1].start()
    grad_copy = pltpu.make_async_copy(grad_hbm, grad_in, load_sem.at[0])
    weights_copy = pltpu.make_async_copy(weights_hbm, held, load_sem.at[4])
    small_copies = [
        pltpu.make_async_copy(len_hbm, len_v, load_sem.at[1]),
        pltpu.make_async_copy(slot_hbm, slot_v, load_sem.at[2]),
        pltpu.make_async_copy(accum_hbm, accum_v, load_sem.at[3]),
    ]

    with jax.named_scope("signal_up"):
        for q in peers[1:]:
            signal(barrier, grp, q)

        @pl.loop(grp + 1, groups)
        def _(g):
            @pl.when(above(g))
            def _():
                signal(barrier, g, lane)

        @pl.when(grp < groups - 1)
        def _():
            for x in range(half):

                @pl.when(lane != 2 * x + 1)
                def _():
                    signal(barrier, groups - 1, 2 * x + 1)

    grad_copy.start()
    for copy in small_copies:
        copy.start()

    with jax.named_scope("barrier"):

        @pl.when(is_top)
        def _():
            pl.semaphore_wait(barrier, devices - 1)

        @pl.when(jnp.logical_not(is_top))
        def _():
            pl.semaphore_wait(barrier, lanes - 2 + (row + 1) * (place + 1))

    with jax.named_scope("signal_down"):

        @pl.loop(0, grp)
        def _(g):
            @pl.when(below(g) & is_far)
            def _():
                signal(far_ready, g, lane)

            @pl.when(below(g) & (grp < near))
            def _():
                signal(near_ready, g, lane)

        if side > 1:

            @pl.when(is_top)
            def _():
                @pl.loop(1, groups - 1)
                def _(i):
                    g = groups - 1 - i

                    @pl.when(is_apart(g))
                    def _():
                        for q in range(lanes):
                            signal(top_ready, g, q)

    with jax.named_scope("look_wait"):
        for copy in look_copies:
            copy.wait()
    for k in range(1, lanes):
        marks_out[k - 1] = marks_in[k].astype(F32).astype(marks_out.dtype)
    a_copies = []
    for k, q in enumerate(peers[1:], 1):
        copy = pltpu.make_async_remote_copy(
            src_ref=marks_out.at[k - 1],
            dst_ref=marks.at[lane],
            send_sem=a_send.at[k - 1],
            recv_sem=a_recv.at[lane],
            device_id=(grp, q),
            device_id_type=MESH,
        )
        copy.start()
        a_copies.append(copy)

    with jax.named_scope("grad_wait"):
        grad_copy.wait()
    weights_copy.start()
    with jax.named_scope("grad_turn"):
        for c in range(embed // 128):
            grad_f32[c] = grad_in[:, c * 128 : (c + 1) * 128].astype(F32)
        for t in range(tables_all):
            for c in range(embed // 128):
                grad_t[t, :, c * 128 : (c + 1) * 128] = grad_f32[
                    c, pl.ds(t, batch, stride=tables_all), :
                ].astype(BF16)
    for copy in small_copies:
        copy.wait()
    pair_copy = pltpu.make_async_remote_copy(
        src_ref=slot_v,
        dst_ref=pair_slot,
        send_sem=e_send,
        recv_sem=e_recv,
        device_id=(grp, lane - core + 1),
        device_id_type=MESH,
    )
    slot_copy = pltpu.make_async_remote_copy(
        src_ref=slot_v,
        dst_ref=shadow_slot.at[core],
        send_sem=f_send,
        recv_sem=f_recv,
        device_id=(jnp.maximum(grp - span, 0), lane - core + 1),
        device_id_type=MESH,
    )

    @pl.when(core == 0)
    def _():
        pair_copy.start()
        pair_slot[...] = jnp.zeros(pair_slot.shape, jnp.int32)

    @pl.when(jnp.logical_not(is_shadow))
    def _():
        shadow_slot[...] = jnp.zeros(shadow_slot.shape, jnp.int32)

    shadow_sums[...] = jnp.zeros(shadow_sums.shape, BF16)

    marks[lane] = marks_in[0].astype(F32).astype(marks.dtype)
    number = iota((slots, batch), 0).astype(F32)

    def take(m):
        total = partial_of(m)
        for h in range(widths):
            part_f[m // 2, pl.ds(m % 2 * widths + h, slots, stride=2 * widths), :] = total[
                :, h * 128 : (h + 1) * 128
            ]

    def marks_from(m, name):
        with jax.named_scope(name):
            pltpu.make_async_copy(marks.at[m], marks.at[m], a_recv.at[m]).wait()

    def settle(x):
        for p in range(groups):
            part[x, p] = part_f[x, p * tile : (p + 1) * tile].astype(BF16)

    def send(p, x):
        pltpu.make_async_remote_copy(
            src_ref=part.at[x, p],
            dst_ref=recv.at[me],
            send_sem=b_send,
            recv_sem=b_recv,
            device_id=(p, 2 * x + 1),
            device_id_type=MESH,
        ).start()

    def send_shadow(p, x):
        pltpu.make_async_remote_copy(
            src_ref=part.at[x, p],
            dst_ref=shadow_in.at[me],
            send_sem=d_send,
            recv_sem=d_recv,
            device_id=(p - span, 2 * x + 1),
            device_id_type=MESH,
        ).start()

    def mine(p, x):
        return leader & (p == grp) & (x == column)

    def each_group(first, last, body):
        if groups <= 16:
            for p in range(first, last):
                body(p)
        else:
            pl.loop(first, last)(body)

    def send_all(first, last, wanted):
        def body(i):
            p = last - 1 + first - i
            for x in range(half):

                @pl.when(wanted(p) & jnp.logical_not(mine(p, x)))
                def _():
                    send(p, x)

        each_group(first, last, body)

    def send_shadows(wanted, columns):
        def body(p):
            for x in columns:
                here = mine(p - span, x)

                @pl.when(wanted(p - span) & jnp.logical_not(here))
                def _():
                    send_shadow(p, x)

                @pl.when(wanted(p - span) & here)
                def _():
                    pltpu.make_async_copy(part.at[x, p], shadow_in.at[me], d_recv).start()

        each_group(near, groups, body)

    def in_line(p):
        return above(p) | below(p) | (p == grp)

    def off_line(p):
        return jnp.logical_not(in_line(p))

    def keep_own():
        @pl.when(leader)
        def _():
            pltpu.make_async_copy(part.at[column, grp], recv.at[me], b_recv).start()

    def near_known():
        with jax.named_scope("near_wait"):

            @pl.when(near_above > 0)
            def _():
                pl.semaphore_wait(near_ready, near_above)

    def far_known():
        with jax.named_scope("far_wait"):

            @pl.when(far_above > 0)
            def _():
                pl.semaphore_wait(far_ready, far_above)

    def rest_known():
        with jax.named_scope("column_wait"):
            pl.semaphore_wait(top_ready, half)

    late = grp >= groups // 2
    take(lane)
    marks_from(partner, "marks_wait1")

    @pl.when(is_far)
    def _():
        slot_copy.start()

    take(partner)
    settle(column)

    @pl.when(late)
    def _():
        near_known()
        far_known()
        pl.when(is_apart(grp))(rest_known)
        send_shadows(lambda p: True, [column])

        def body(p):
            @pl.when(jnp.logical_not(leader & (p == grp)))
            def _():
                send(p, column)

        each_group(0, groups, body)
        keep_own()

    for x in others:
        marks_from(2 * x + 1, "marks_wait2")
        take(2 * x + 1)
    for x in others:
        marks_from(2 * x, "marks_wait3")
        take(2 * x)
    for x in others:
        settle(x)

    @pl.when(late)
    def _():
        for x in others:
            each_group(0, groups, lambda p: send(p, x))
            each_group(near, groups, lambda p: send_shadow(p, x))

    @pl.when(jnp.logical_not(late))
    def _():
        near_known()
        send_shadows(in_line, range(half))
        send_all(0, near, in_line)
        keep_own()
        far_known()
        send_all(near, groups, in_line)

        @pl.when(is_apart(grp))
        def _():
            rest_known()
            send_shadows(off_line, range(half))
            send_all(0, groups, off_line)

    with jax.named_scope("sent"):
        pass

    two = 2 * slots
    which = iota((two, groups), 0)
    span_of = tables * rows

    def named_rows(low, high):
        low, high = low.astype(F32), high.astype(F32)
        pick = jnp.zeros((two, groups), F32)
        for k in range(per_peer):
            pick = jnp.where(which % (2 * per_peer) == 2 * k, low[k : k + 1, :], pick)
            pick = jnp.where(which % (2 * per_peer) == 2 * k + 1, high[k : k + 1, :], pick)
        pick = jnp.where(which // (2 * per_peer) == iota((two, groups), 1), pick, 0.0)
        return jnp.sum(pick, axis=1, keepdims=True)

    @pl.when(leader)
    def _():
        pair_copy.wait_recv()

    @pl.when(is_shadow)
    def _():
        pltpu.make_async_copy(shadow_slot, shadow_slot, f_recv).wait()

    own_slot, other_slot = slot_v[...], pair_slot[...] + span_of
    target_col = jnp.concatenate(
        [
            named_rows(
                jnp.where(leader, other_slot, own_slot), jnp.where(leader, own_slot, other_slot)
            ),
            named_rows(shadow_slot[0] + 2 * span_of, shadow_slot[1] + 3 * span_of),
        ],
        axis=0,
    )
    i_id, j_id = iota((2 * two, 2 * two), 0), iota((2 * two, 2 * two), 1)
    target_row = jnp.sum(jnp.where(i_id == j_id, target_col, 0.0), axis=0, keepdims=True)
    same = target_col == target_row
    first_col = jnp.sum(jnp.where(same & (j_id < i_id), 1.0, 0.0), axis=1, keepdims=True) == 0.0
    first_row = jnp.sum(jnp.where(same & (i_id < j_id), 1.0, 0.0), axis=0, keepdims=True) == 0.0
    is_own = (target_row < span_of) & first_row
    place_row = jnp.where(is_own, target_row, -1.0)
    packed[place_base : place_base + 1, :two] = place_row[:, :two]
    wide = (2 * two, widths * 2 * two)
    wide_i, wide_j = iota(wide, 0), iota(wide, 1)
    spread_row = jnp.sum(
        jnp.where(wide_i == wide_j // widths, target_col, 0.0), axis=0, keepdims=True
    )
    picks = [
        jnp.where((target_col == spread_row) & (wide_j % widths == h), 1.0, 0.0).astype(BF16)
        for h in range(widths)
    ]

    hits = []
    accum_col = jnp.zeros((two, 1), F32)
    for t in range(tables):
        hit = target_col[:two] == (iota((two, rows), 1) + t * rows).astype(F32)
        hits.append(hit)
        accum_col += jnp.sum(
            jnp.where(hit, accum_v[t : t + 1, :], 0.0), axis=1, keepdims=True
        )

    def gather(source):
        group_sums = []
        for g in range(groups):
            group_sum = source[g * lanes].astype(F32)
            for q in range(1, lanes):
                group_sum += source[g * lanes + q].astype(F32)
            group_sums.append(group_sum)
        return jnp.concatenate(group_sums, axis=0).astype(BF16)

    sums_copy = pltpu.make_async_remote_copy(
        src_ref=sums,
        dst_ref=sums,
        send_sem=g_send,
        recv_sem=g_recv,
        device_id=(grp, lane - core),
        device_id_type=MESH,
    )

    @pl.when(is_shadow)
    def _():
        with jax.named_scope("shadow_wait"):
            pltpu.make_async_copy(shadow_in, shadow_in, d_recv).wait()
        shadow_sums[...] = gather(shadow_in)

    with jax.named_scope("sums_wait"):

        @pl.when(leader)
        def _():
            pltpu.make_async_copy(recv, recv, b_recv).wait()
            sums[...] = gather(recv)
            sums_copy.start()

        @pl.when(core == 0)
        def _():
            sums_copy.wait_recv()

    all_sums = jnp.concatenate([sums[...], shadow_sums[...]], axis=0)
    pieces = [jnp.dot(pick, all_sums, preferred_element_type=F32) for pick in picks]
    squares = sum(piece * piece for piece in pieces)
    norm_out[...] = jnp.sum(jnp.where(first_col, squares, 0.0), axis=0, keepdims=True)

    def tell(far):
        pltpu.make_async_remote_copy(
            src_ref=norm_out,
            dst_ref=norm_in.at[grp * half + column],
            send_sem=c_send,
            recv_sem=c_recv,
            device_id=(far // lanes, far % lanes),
            device_id_type=MESH,
        ).start()

    @pl.when(tells)
    def _():
        if devices <= 64:
            for d in range(1, devices):
                tell((me + sign * d + devices) % devices)
        else:
            each(devices - 1, lambda i: tell((me + i + 1) % devices))
        pltpu.make_async_copy(norm_out, norm_in.at[grp * half + column], c_recv).start()

    grads = jnp.concatenate([piece[:two] for piece in pieces], axis=1)
    square_col = jnp.sum(squares[:two], axis=1, keepdims=True) * (1.0 / embed)
    square_first = jnp.where(first_col[:two], square_col, 0.0)
    square_rows = [
        jnp.sum(jnp.where(hit, square_first, 0.0), axis=0, keepdims=True) for hit in hits
    ]
    for copy in a_copies:
        copy.wait_send()

    def sent(buffer, count, semaphore):
        piece = buffer.at[pl.ds(0, count)]
        pltpu.make_async_copy(piece, piece, semaphore).wait()

    pl.when(leader)(lambda: sent(recv, groups * half - 1, b_send))
    pl.when(core == 0)(lambda: sent(recv, groups * half, b_send))
    if span > 0:
        pl.when(is_shadow)(lambda: sent(shadow_in, span * half - 1, d_send))
        pl.when(jnp.logical_not(is_shadow))(lambda: sent(shadow_in, span * half, d_send))

    @pl.when(is_far)
    def _():
        slot_copy.wait_send()

    @pl.when(core == 0)
    def _():
        pair_copy.wait_send()

    @pl.when(leader)
    def _():
        sums_copy.wait_send()

    with jax.named_scope("norm_wait"):
        told = norm_in.at[pl.ds(0, near * half)]
        pltpu.make_async_copy(told, told, c_recv).wait()
    weights_copy.wait()
    norm_total = jnp.sum(jnp.sum(norm_in[: near * half], axis=0), axis=1, keepdims=True)
    clip_limit = 0.5 * math.sqrt(devices * slots * embed)
    clip = clip_limit / jnp.maximum(jnp.sqrt(norm_total), clip_limit)
    for t in range(tables):
        packed[accum_base + t : accum_base + t + 1, :rows] = accum_v[t : t + 1, :] + clip * clip * square_rows[t]
    new_accum_col = accum_col + clip * clip * square_col
    delta = LEARN_RATE * clip * grads / (jnp.sqrt(new_accum_col) + EPSILON)
    packed[:two, :embed] = delta

    @pl.when(tells)
    def _():
        told = norm_in.at[pl.ds(0, devices - 1)]
        pltpu.make_async_copy(told, told, c_send).wait()


def update_kernel(
    chunk, slots, place_base, accum_base, weights, packed, wout, aout, held, accum, sems, accum_sem
):
    accum[...] = packed[accum_base : accum_base + accum.shape[0], : accum.shape[1]]
    accum_copy = pltpu.make_async_copy(accum, aout, accum_sem)
    accum_copy.start()
    delta = packed[:slots, : weights.shape[2]]
    high = delta.astype(BF16)
    deltas = jnp.concatenate([high, (delta - high.astype(F32)).astype(BF16)], axis=0)
    place_row = packed[place_base : place_base + 1, :slots]
    place_row = jnp.concatenate([place_row, place_row], axis=1)
    tables, rows = weights.shape[0], weights.shape[1]
    copies = []
    for t in range(tables):
        for c in range(0, rows, chunk):
            row_id = (iota((chunk, 1), 0) + (t * rows + c)).astype(F32)
            place = jnp.where(row_id == place_row, 1.0, 0.0).astype(BF16)
            held[t, c : c + chunk] = weights[t, c : c + chunk] - jnp.dot(
                place, deltas, preferred_element_type=F32
            )
            copies.append(
                pltpu.make_async_copy(
                    held.at[t, pl.ds(c, chunk)],
                    wout.at[t, pl.ds(c, chunk)],
                    sems.at[len(copies)],
                )
            )
            copies[-1].start()
    for copy in copies:
        copy.wait()
    accum_copy.wait()


def per_device(groups, lanes, grad_pooled, bag_len, lookup_slot, slot_row, weights, accum):
    batch, tables_all, embed = grad_pooled.shape
    samples, tables, depth = lookup_slot.shape
    rows = accum.shape[1]
    per_peer = slot_row.shape[3]
    devices = groups * lanes
    slots = groups * per_peer
    mark_type = BF16 if slots <= 256 else F32
    half = lanes // 2
    tile = 2 * per_peer * (embed // 128)
    place_base = -(-2 * slots // 8) * 8
    accum_base = place_base + 8
    packed_shape = (accum_base + -(-tables // 8) * 8, max(embed, rows, 2 * slots))
    anywhere = pl.BlockSpec(memory_space=pl.ANY)
    vmem = pl.BlockSpec(memory_space=pltpu.VMEM)
    packed, held = pl.pallas_call(
        functools.partial(kernel, groups, lanes, place_base, accum_base),
        out_shape=(
            jax.ShapeDtypeStruct(packed_shape, F32),
            jax.ShapeDtypeStruct(weights.shape, F32),
        ),
        in_specs=[pl.BlockSpec(memory_space=pltpu.HBM)] * 6,
        out_specs=(vmem, vmem),
        cost_estimate=pl.CostEstimate(
            flops=8 * slots * batch * tables_all * embed,
            bytes_accessed=32 * batch * tables_all * embed,
            transcendentals=0,
        ),
        scratch_shapes=[
            pltpu.VMEM((batch * tables_all, embed), BF16),
            pltpu.VMEM((embed // 128, batch * tables_all, 128), F32),
            pltpu.VMEM((tables_all, batch, embed), BF16),
            pltpu.VMEM((tables_all, batch), jnp.int32),
            pltpu.VMEM((lanes, tables, depth, batch), mark_type),
            pltpu.VMEM((lanes, tables, depth, batch), jnp.int32),
            pltpu.VMEM((lanes - 1, tables, depth, batch), mark_type),
            pltpu.VMEM((per_peer, groups), jnp.int32),
            pltpu.VMEM((tables, rows), F32),
            pltpu.VMEM((half, groups * tile, 128), F32),
            pltpu.VMEM((half, groups, tile, 128), BF16),
            pltpu.VMEM((devices, tile, 128), BF16),
            pltpu.VMEM((groups * tile, 128), BF16),
            pltpu.VMEM((groups * tile, 128), BF16),
            pltpu.VMEM((1, 128), F32),
            pltpu.VMEM((devices, 1, 128), F32),
            pltpu.SemaphoreType.DMA((5,)),
            pltpu.SemaphoreType.DMA((lanes,)),
            pltpu.SemaphoreType.DMA((lanes - 1,)),
            pltpu.SemaphoreType.DMA((lanes,)),
            pltpu.SemaphoreType.DMA,
            pltpu.SemaphoreType.DMA,
            pltpu.SemaphoreType.DMA,
            pltpu.SemaphoreType.DMA,
            pltpu.SemaphoreType.REGULAR,
            pltpu.SemaphoreType.REGULAR,
            pltpu.SemaphoreType.REGULAR,
            pltpu.VMEM((devices, tile, 128), BF16),
            pltpu.VMEM((per_peer, groups), jnp.int32),
            pltpu.VMEM((2, per_peer, groups), jnp.int32),
            pltpu.SemaphoreType.DMA,
            pltpu.SemaphoreType.DMA,
            pltpu.SemaphoreType.DMA,
            pltpu.SemaphoreType.DMA,
            pltpu.SemaphoreType.DMA,
            pltpu.SemaphoreType.DMA,
            pltpu.SemaphoreType.DMA,
            pltpu.SemaphoreType.DMA,
        ],
        compiler_params=pltpu.CompilerParams(
            collective_id=0, has_side_effects=True, vmem_limit_bytes=32 << 20
        ),
    )(
        *(
            pltpu.with_memory_space_constraint(operand, pltpu.HBM)
            for operand in (
                grad_pooled.reshape(batch * tables_all, embed),
                bag_len.T,
                jnp.transpose(lookup_slot, (1, 2, 0)),
                slot_row.reshape(groups, per_peer).T,
                accum,
                weights,
            )
        )
    )
    chunk = min(rows, 128)
    return pl.pallas_call(
        functools.partial(update_kernel, chunk, 2 * slots, place_base, accum_base),
        out_shape=(
            jax.ShapeDtypeStruct(weights.shape, F32),
            jax.ShapeDtypeStruct(accum.shape, F32),
        ),
        in_specs=[vmem, vmem],
        out_specs=(anywhere, anywhere),
        scratch_shapes=[
            pltpu.VMEM(weights.shape, F32),
            pltpu.VMEM(accum.shape, F32),
            pltpu.SemaphoreType.DMA((tables * (rows // chunk),)),
            pltpu.SemaphoreType.DMA,
        ],
        compiler_params=pltpu.CompilerParams(vmem_limit_bytes=8 << 20),
    )(held, packed)


def solution(mesh):
    placed = (
        P(("grp", "lane"), None, None),
        P(("grp", "lane"), None),
        P("grp", "lane", None),
        P("grp", "lane", None, None),
        P("lane", "grp", None),
        P("lane", "grp"),
    )
    return jax.shard_map(
        functools.partial(per_device, mesh.shape["grp"], mesh.shape["lane"]),
        mesh=mesh,
        in_specs=placed,
        out_specs=(P("lane", "grp", None), P("lane", "grp")),
        check_vma=False,
    )
```

```python
import functools
import math

import jax
import jax.numpy as jnp
from jax import lax
from jax.experimental import pallas as pl
from jax.experimental.pallas import tpu as pltpu
from jax.sharding import PartitionSpec as P

MESH = pl.DeviceIdType.MESH
LEARN_RATE = 0.3
EPSILON = 1e-06
SIDE = 2
F32 = jnp.float32
BF16 = jnp.bfloat16


def each(count, body):
    if count <= 64:
        for i in range(count):
            body(i)
    else:

        def step(i, carry):
            body(i)
            return carry

        lax.fori_loop(0, count, step, 0)


def iota(shape, dim):
    return lax.broadcasted_iota(jnp.int32, shape, dim)


def kernel(
    groups,
    lanes,
    grad_hbm,
    len_hbm,
    look_hbm,
    slot_hbm,
    accum_hbm,
    weights_hbm,
    packed,
    held,
    place_out,
    delta_out,
    grad_in,
    grad_f32,
    grad_t,
    len_v,
    marks,
    marks_in,
    marks_out,
    slot_v,
    accum_v,
    part_f,
    part,
    recv,
    sums,
    shadow_sums,
    norm_out,
    norm_in,
    load_sem,
    look_sem,
    a_send,
    a_recv,
    b_send,
    b_recv,
    c_send,
    c_recv,
    near_ready,
    far_ready,
    top_ready,
    shadow_in,
    pair_slot,
    shadow_slot,
    d_send,
    d_recv,
    e_send,
    e_recv,
    f_send,
    f_recv,
    g_send,
    g_recv,
):
    devices = groups * lanes
    per_peer, embed = slot_v.shape[0], grad_t.shape[2]
    slots = groups * per_peer
    tables_all, batch = grad_t.shape[0], grad_t.shape[1]
    tables = tables_all // lanes
    depth = marks.shape[2]
    rows = accum_v.shape[1]
    grp = lax.axis_index("grp")
    lane = lax.axis_index("lane")
    me = grp * lanes + lane
    sign = 2 * (grp // (groups // 2)) - 1

    def partial_of(m):
        highs, lows = [], []
        for t in range(tables):
            mark = marks[m, t].astype(F32)
            count = jnp.zeros((slots, batch), F32)
            for j in range(depth):
                count += jnp.where(mark[j : j + 1, :] == number, 1.0, 0.0)
            length = len_v[pl.ds(m * tables + t, 1), :].astype(F32)
            factor = count / length
            high = factor.astype(BF16)
            highs.append(high)
            lows.append((factor - high.astype(F32)).astype(BF16))
        factors = jnp.concatenate(
            [jnp.concatenate(highs, axis=1), jnp.concatenate(lows, axis=1)], axis=0
        )
        values = grad_t[pl.ds(m * tables, tables)].reshape(tables * batch, embed)
        both = jnp.dot(factors, values, preferred_element_type=F32)
        return both[:slots] + both[slots:]

    side = SIDE if groups % (4 * SIDE) == 0 else 1
    depth_all = groups // side
    span = depth_all // 4 * side
    near = groups - span
    near_depth = near // side
    far_depth = depth_all - near_depth
    row, place = grp // side, grp % side
    rows_above, places_above = depth_all - row, side - place
    near_above = jnp.maximum(near_depth - row, 0) * places_above - jnp.where(grp < near, 1, 0)
    far_above = jnp.minimum(rows_above, far_depth) * places_above - jnp.where(grp < near, 0, 1)

    def is_apart(g):
        r, p = g // side, g % side
        return ((r > 0) & (p < side - 1)) | ((r < depth_all - 1) & (p > 0))


    def above(g):
        return (g // side >= row) & (g % side >= place) & (g != grp)

    def below(g):
        return (g // side <= row) & (g % side <= place) & (g != grp)

    half = lanes // 2
    column, core = lane // 2, lane % 2
    leader = core == 1
    widths = embed // 128
    tile = recv.shape[1]
    is_far = grp >= near
    is_top = leader & (grp == groups - 1)
    tells = leader & (grp < near)
    is_shadow = leader & (grp >= near - span) & (grp < near)

    barrier = pltpu.get_barrier_semaphore()
    partner = lane + 1 - 2 * core
    others = [lax.rem(column + d, half) for d in range(1, half)]
    peers = [lane] + [2 * x for x in others] + [2 * x + 1 for x in others] + [partner]

    def signal(semaphore, g, q):
        pl.semaphore_signal(semaphore, inc=1, device_id=(g, q), device_id_type=MESH)

    look_copies = []
    for k, q in enumerate(peers):
        src = look_hbm.at[:, :, pl.ds(pl.multiple_of(q * batch, batch), batch)]
        look_copies.append(pltpu.make_async_copy(src, marks_in.at[k], look_sem.at[k]))
        look_copies[-1].start()
    grad_copy = pltpu.make_async_copy(grad_hbm, grad_in, load_sem.at[0])
    weights_copy = pltpu.make_async_copy(weights_hbm, held, load_sem.at[4])
    small_copies = [
        pltpu.make_async_copy(len_hbm, len_v, load_sem.at[1]),
        pltpu.make_async_copy(slot_hbm, slot_v, load_sem.at[2]),
        pltpu.make_async_copy(accum_hbm, accum_v, load_sem.at[3]),
    ]

    with jax.named_scope("signal_up"):
        for q in peers[1:]:
            signal(barrier, grp, q)

        @pl.loop(grp + 1, groups)
        def _(g):
            @pl.when(above(g))
            def _():
                signal(barrier, g, lane)

        @pl.when(grp < groups - 1)
        def _():
            for x in range(half):

                @pl.when(lane != 2 * x + 1)
                def _():
                    signal(barrier, groups - 1, 2 * x + 1)

    grad_copy.start()
    for copy in small_copies:
        copy.start()

    with jax.named_scope("barrier"):

        @pl.when(is_top)
        def _():
            pl.semaphore_wait(barrier, devices - 1)

        @pl.when(jnp.logical_not(is_top))
        def _():
            pl.semaphore_wait(barrier, lanes - 2 + (row + 1) * (place + 1))

    with jax.named_scope("signal_down"):

        @pl.loop(0, grp)
        def _(g):
            @pl.when(below(g) & is_far)
            def _():
                signal(far_ready, g, lane)

            @pl.when(below(g) & (grp < near))
            def _():
                signal(near_ready, g, lane)

        if side > 1:

            @pl.when(is_top)
            def _():
                @pl.loop(1, groups - 1)
                def _(i):
                    g = groups - 1 - i

                    @pl.when(is_apart(g))
                    def _():
                        for q in range(lanes):
                            signal(top_ready, g, q)

    with jax.named_scope("look_wait"):
        for copy in look_copies:
            copy.wait()
    for k in range(1, lanes):
        marks_out[k - 1] = marks_in[k].astype(F32).astype(marks_out.dtype)
    a_copies = []
    for k, q in enumerate(peers[1:], 1):
        copy = pltpu.make_async_remote_copy(
            src_ref=marks_out.at[k - 1],
            dst_ref=marks.at[lane],
            send_sem=a_send.at[k - 1],
            recv_sem=a_recv.at[lane],
            device_id=(grp, q),
            device_id_type=MESH,
        )
        copy.start()
        a_copies.append(copy)

    with jax.named_scope("grad_wait"):
        grad_copy.wait()
    weights_copy.start()
    with jax.named_scope("grad_turn"):
        for c in range(embed // 128):
            grad_f32[c] = grad_in[:, c * 128 : (c + 1) * 128].astype(F32)
        for t in range(tables_all):
            for c in range(embed // 128):
                grad_t[t, :, c * 128 : (c + 1) * 128] = grad_f32[
                    c, pl.ds(t, batch, stride=tables_all), :
                ].astype(BF16)
    for copy in small_copies:
        copy.wait()
    pair_copy = pltpu.make_async_remote_copy(
        src_ref=slot_v,
        dst_ref=pair_slot,
        send_sem=e_send,
        recv_sem=e_recv,
        device_id=(grp, lane - core + 1),
        device_id_type=MESH,
    )
    slot_copy = pltpu.make_async_remote_copy(
        src_ref=slot_v,
        dst_ref=shadow_slot.at[core],
        send_sem=f_send,
        recv_sem=f_recv,
        device_id=(jnp.maximum(grp - span, 0), lane - core + 1),
        device_id_type=MESH,
    )

    @pl.when(core == 0)
    def _():
        pair_copy.start()
        pair_slot[...] = jnp.zeros(pair_slot.shape, jnp.int32)

    @pl.when(jnp.logical_not(is_shadow))
    def _():
        shadow_slot[...] = jnp.zeros(shadow_slot.shape, jnp.int32)

    shadow_sums[...] = jnp.zeros(shadow_sums.shape, BF16)

    marks[lane] = marks_in[0].astype(F32).astype(marks.dtype)
    number = iota((slots, batch), 0).astype(F32)

    def take(m):
        total = partial_of(m)
        for h in range(widths):
            part_f[m // 2, pl.ds(m % 2 * widths + h, slots, stride=2 * widths), :] = total[
                :, h * 128 : (h + 1) * 128
            ]

    def marks_from(m, name):
        with jax.named_scope(name):
            pltpu.make_async_copy(marks.at[m], marks.at[m], a_recv.at[m]).wait()

    def settle(x):
        for p in range(groups):
            part[x, p] = part_f[x, p * tile : (p + 1) * tile].astype(BF16)

    def send(p, x):
        pltpu.make_async_remote_copy(
            src_ref=part.at[x, p],
            dst_ref=recv.at[me],
            send_sem=b_send,
            recv_sem=b_recv,
            device_id=(p, 2 * x + 1),
            device_id_type=MESH,
        ).start()

    def send_shadow(p, x):
        pltpu.make_async_remote_copy(
            src_ref=part.at[x, p],
            dst_ref=shadow_in.at[me],
            send_sem=d_send,
            recv_sem=d_recv,
            device_id=(p - span, 2 * x + 1),
            device_id_type=MESH,
        ).start()

    def mine(p, x):
        return leader & (p == grp) & (x == column)

    def each_group(first, last, body):
        if groups <= 16:
            for p in range(first, last):
                body(p)
        else:
            pl.loop(first, last)(body)

    def send_all(first, last, wanted):
        def body(i):
            p = last - 1 + first - i
            for x in range(half):

                @pl.when(wanted(p) & jnp.logical_not(mine(p, x)))
                def _():
                    send(p, x)

        each_group(first, last, body)

    def send_shadows(wanted, columns):
        def body(p):
            for x in columns:
                here = mine(p - span, x)

                @pl.when(wanted(p - span) & jnp.logical_not(here))
                def _():
                    send_shadow(p, x)

                @pl.when(wanted(p - span) & here)
                def _():
                    pltpu.make_async_copy(part.at[x, p], shadow_in.at[me], d_recv).start()

        each_group(near, groups, body)

    def in_line(p):
        return above(p) | below(p) | (p == grp)

    def off_line(p):
        return jnp.logical_not(in_line(p))

    def keep_own():
        @pl.when(leader)
        def _():
            pltpu.make_async_copy(part.at[column, grp], recv.at[me], b_recv).start()

    def near_known():
        with jax.named_scope("near_wait"):

            @pl.when(near_above > 0)
            def _():
                pl.semaphore_wait(near_ready, near_above)

    def far_known():
        with jax.named_scope("far_wait"):

            @pl.when(far_above > 0)
            def _():
                pl.semaphore_wait(far_ready, far_above)

    def rest_known():
        with jax.named_scope("column_wait"):
            pl.semaphore_wait(top_ready, half)

    late = grp >= groups // 2
    take(lane)
    marks_from(partner, "marks_wait1")

    @pl.when(is_far)
    def _():
        slot_copy.start()

    take(partner)
    settle(column)

    @pl.when(late)
    def _():
        near_known()
        far_known()
        pl.when(is_apart(grp))(rest_known)
        send_shadows(lambda p: True, [column])

        def body(p):
            @pl.when(jnp.logical_not(leader & (p == grp)))
            def _():
                send(p, column)

        each_group(0, groups, body)
        keep_own()

    for x in others:
        marks_from(2 * x + 1, "marks_wait2")
        take(2 * x + 1)
    for x in others:
        marks_from(2 * x, "marks_wait3")
        take(2 * x)
    for x in others:
        settle(x)

    @pl.when(late)
    def _():
        for x in others:
            each_group(0, groups, lambda p: send(p, x))
            each_group(near, groups, lambda p: send_shadow(p, x))

    @pl.when(jnp.logical_not(late))
    def _():
        near_known()
        send_shadows(in_line, range(half))
        send_all(0, near, in_line)
        keep_own()
        far_known()
        send_all(near, groups, in_line)

        @pl.when(is_apart(grp))
        def _():
            rest_known()
            send_shadows(off_line, range(half))
            send_all(0, groups, off_line)

    with jax.named_scope("sent"):
        pass

    two = 2 * slots
    which = iota((two, groups), 0)
    span_of = tables * rows

    def named_rows(low, high):
        low, high = low.astype(F32), high.astype(F32)
        pick = jnp.zeros((two, groups), F32)
        for k in range(per_peer):
            pick = jnp.where(which % (2 * per_peer) == 2 * k, low[k : k + 1, :], pick)
            pick = jnp.where(which % (2 * per_peer) == 2 * k + 1, high[k : k + 1, :], pick)
        pick = jnp.where(which // (2 * per_peer) == iota((two, groups), 1), pick, 0.0)
        return jnp.sum(pick, axis=1, keepdims=True)

    @pl.when(leader)
    def _():
        pair_copy.wait_recv()

    @pl.when(is_shadow)
    def _():
        pltpu.make_async_copy(shadow_slot, shadow_slot, f_recv).wait()

    own_slot, other_slot = slot_v[...], pair_slot[...] + span_of
    target_col = jnp.concatenate(
        [
            named_rows(
                jnp.where(leader, other_slot, own_slot), jnp.where(leader, own_slot, other_slot)
            ),
            named_rows(shadow_slot[0] + 2 * span_of, shadow_slot[1] + 3 * span_of),
        ],
        axis=0,
    )
    i_id, j_id = iota((2 * two, 2 * two), 0), iota((2 * two, 2 * two), 1)
    target_row = jnp.sum(jnp.where(i_id == j_id, target_col, 0.0), axis=0, keepdims=True)
    same = target_col == target_row
    first_col = jnp.sum(jnp.where(same & (j_id < i_id), 1.0, 0.0), axis=1, keepdims=True) == 0.0
    first_row = jnp.sum(jnp.where(same & (i_id < j_id), 1.0, 0.0), axis=0, keepdims=True) == 0.0
    is_own = (target_row < span_of) & first_row
    place_row = jnp.where(is_own, target_row, -1.0)[:, :two]
    place_row = jnp.concatenate([place_row, place_row], axis=1)
    for r in range(0, span_of, 128):
        row_id = (iota((128, 1), 0) + r).astype(F32)
        place_out[r : r + 128] = jnp.where(row_id == place_row, 1.0, 0.0).astype(BF16)
    wide = (2 * two, widths * 2 * two)
    wide_i, wide_j = iota(wide, 0), iota(wide, 1)
    spread_row = jnp.sum(
        jnp.where(wide_i == wide_j // widths, target_col, 0.0), axis=0, keepdims=True
    )
    picks = [
        jnp.where((target_col == spread_row) & (wide_j % widths == h), 1.0, 0.0).astype(BF16)
        for h in range(widths)
    ]

    hits = []
    accum_col = jnp.zeros((two, 1), F32)
    for t in range(tables):
        hit = target_col[:two] == (iota((two, rows), 1) + t * rows).astype(F32)
        hits.append(hit)
        accum_col += jnp.sum(
            jnp.where(hit, accum_v[t : t + 1, :], 0.0), axis=1, keepdims=True
        )

    def gather(source):
        group_sums = []
        for g in range(groups):
            group_sum = source[g * lanes].astype(F32)
            for q in range(1, lanes):
                group_sum += source[g * lanes + q].astype(F32)
            group_sums.append(group_sum)
        return jnp.concatenate(group_sums, axis=0).astype(BF16)

    sums_copy = pltpu.make_async_remote_copy(
        src_ref=sums,
        dst_ref=sums,
        send_sem=g_send,
        recv_sem=g_recv,
        device_id=(grp, lane - core),
        device_id_type=MESH,
    )

    @pl.when(is_shadow)
    def _():
        with jax.named_scope("shadow_wait"):
            pltpu.make_async_copy(shadow_in, shadow_in, d_recv).wait()
        shadow_sums[...] = gather(shadow_in)

    with jax.named_scope("sums_wait"):

        @pl.when(leader)
        def _():
            pltpu.make_async_copy(recv, recv, b_recv).wait()
            sums[...] = gather(recv)
            sums_copy.start()

        @pl.when(core == 0)
        def _():
            sums_copy.wait_recv()

    all_sums = jnp.concatenate([sums[...], shadow_sums[...]], axis=0)
    pieces = [jnp.dot(pick, all_sums, preferred_element_type=F32) for pick in picks]
    squares = sum(piece * piece for piece in pieces)
    norm_out[...] = jnp.sum(jnp.where(first_col, squares, 0.0), axis=0, keepdims=True)

    def tell(far):
        pltpu.make_async_remote_copy(
            src_ref=norm_out,
            dst_ref=norm_in.at[grp * half + column],
            send_sem=c_send,
            recv_sem=c_recv,
            device_id=(far // lanes, far % lanes),
            device_id_type=MESH,
        ).start()

    @pl.when(tells)
    def _():
        each(devices - 1, lambda i: tell(jnp.where(i < me, i, i + 1)))
        pltpu.make_async_copy(norm_out, norm_in.at[grp * half + column], c_recv).start()

    grads = jnp.concatenate([piece[:two] for piece in pieces], axis=1)
    square_col = jnp.sum(squares[:two], axis=1, keepdims=True) * (1.0 / embed)
    square_first = jnp.where(first_col[:two], square_col, 0.0)
    square_rows = [
        jnp.sum(jnp.where(hit, square_first, 0.0), axis=0, keepdims=True) for hit in hits
    ]
    for copy in a_copies:
        copy.wait_send()

    def sent(buffer, count, semaphore):
        piece = buffer.at[pl.ds(0, count)]
        pltpu.make_async_copy(piece, piece, semaphore).wait()

    pl.when(leader)(lambda: sent(recv, groups * half - 1, b_send))
    pl.when(core == 0)(lambda: sent(recv, groups * half, b_send))
    if span > 0:
        pl.when(is_shadow)(lambda: sent(shadow_in, span * half - 1, d_send))
        pl.when(jnp.logical_not(is_shadow))(lambda: sent(shadow_in, span * half, d_send))

    @pl.when(is_far)
    def _():
        slot_copy.wait_send()

    @pl.when(core == 0)
    def _():
        pair_copy.wait_send()

    @pl.when(leader)
    def _():
        sums_copy.wait_send()

    with jax.named_scope("norm_wait"):
        told = norm_in.at[pl.ds(0, near * half)]
        pltpu.make_async_copy(told, told, c_recv).wait()
    weights_copy.wait()
    norm_total = jnp.sum(jnp.sum(norm_in[: near * half], axis=0), axis=1, keepdims=True)
    clip_limit = 0.25 * devices * slots * embed
    clip_square = clip_limit / jnp.maximum(norm_total, clip_limit)
    for t in range(tables):
        packed[t : t + 1, :] = accum_v[t : t + 1, :] + clip_square * square_rows[t]
    new_accum_col = accum_col + clip_square * square_col
    rate = LEARN_RATE * jnp.sqrt(clip_square) / (jnp.sqrt(new_accum_col) + EPSILON)
    delta = rate * grads
    high = delta.astype(BF16)
    delta_out[:two] = high
    delta_out[two:] = (delta - high.astype(F32)).astype(BF16)

    @pl.when(tells)
    def _():
        told = norm_in.at[pl.ds(0, devices - 1)]
        pltpu.make_async_copy(told, told, c_send).wait()


def update_kernel(chunk, weights, place, deltas, packed, wout, aout, held, accum, sems, accum_sem):
    tables, rows = weights.shape[0], weights.shape[1]
    copies = []
    for t in range(tables):
        for c in range(0, rows, chunk):
            held[t, c : c + chunk] = weights[t, c : c + chunk] - jnp.dot(
                place[t * rows + c : t * rows + c + chunk],
                deltas[...],
                preferred_element_type=F32,
            )
            copies.append(
                pltpu.make_async_copy(
                    held.at[t, pl.ds(c, chunk)],
                    wout.at[t, pl.ds(c, chunk)],
                    sems.at[len(copies)],
                )
            )
            copies[-1].start()
    accum[...] = packed[...]
    accum_copy = pltpu.make_async_copy(accum, aout, accum_sem)
    accum_copy.start()
    for copy in copies:
        copy.wait()
    accum_copy.wait()


def per_device(groups, lanes, grad_pooled, bag_len, lookup_slot, slot_row, weights, accum):
    batch, tables_all, embed = grad_pooled.shape
    samples, tables, depth = lookup_slot.shape
    rows = accum.shape[1]
    per_peer = slot_row.shape[3]
    devices = groups * lanes
    slots = groups * per_peer
    mark_type = BF16 if slots <= 256 else F32
    half = lanes // 2
    tile = 2 * per_peer * (embed // 128)
    anywhere = pl.BlockSpec(memory_space=pl.ANY)
    vmem = pl.BlockSpec(memory_space=pltpu.VMEM)
    packed, held, place, deltas = pl.pallas_call(
        functools.partial(kernel, groups, lanes),
        out_shape=(
            jax.ShapeDtypeStruct(accum.shape, F32),
            jax.ShapeDtypeStruct(weights.shape, F32),
            jax.ShapeDtypeStruct((tables * rows, 4 * slots), BF16),
            jax.ShapeDtypeStruct((4 * slots, embed), BF16),
        ),
        in_specs=[pl.BlockSpec(memory_space=pltpu.HBM)] * 6,
        out_specs=(vmem,) * 4,
        cost_estimate=pl.CostEstimate(
            flops=8 * slots * batch * tables_all * embed,
            bytes_accessed=32 * batch * tables_all * embed,
            transcendentals=0,
        ),
        scratch_shapes=[
            pltpu.VMEM((batch * tables_all, embed), BF16),
            pltpu.VMEM((embed // 128, batch * tables_all, 128), F32),
            pltpu.VMEM((tables_all, batch, embed), BF16),
            pltpu.VMEM((tables_all, batch), jnp.int32),
            pltpu.VMEM((lanes, tables, depth, batch), mark_type),
            pltpu.VMEM((lanes, tables, depth, batch), jnp.int32),
            pltpu.VMEM((lanes - 1, tables, depth, batch), mark_type),
            pltpu.VMEM((per_peer, groups), jnp.int32),
            pltpu.VMEM((tables, rows), F32),
            pltpu.VMEM((half, groups * tile, 128), F32),
            pltpu.VMEM((half, groups, tile, 128), BF16),
            pltpu.VMEM((devices, tile, 128), BF16),
            pltpu.VMEM((groups * tile, 128), BF16),
            pltpu.VMEM((groups * tile, 128), BF16),
            pltpu.VMEM((1, 128), F32),
            pltpu.VMEM((devices, 1, 128), F32),
            pltpu.SemaphoreType.DMA((5,)),
            pltpu.SemaphoreType.DMA((lanes,)),
            pltpu.SemaphoreType.DMA((lanes - 1,)),
            pltpu.SemaphoreType.DMA((lanes,)),
            pltpu.SemaphoreType.DMA,
            pltpu.SemaphoreType.DMA,
            pltpu.SemaphoreType.DMA,
            pltpu.SemaphoreType.DMA,
            pltpu.SemaphoreType.REGULAR,
            pltpu.SemaphoreType.REGULAR,
            pltpu.SemaphoreType.REGULAR,
            pltpu.VMEM((devices, tile, 128), BF16),
            pltpu.VMEM((per_peer, groups), jnp.int32),
            pltpu.VMEM((2, per_peer, groups), jnp.int32),
            pltpu.SemaphoreType.DMA,
            pltpu.SemaphoreType.DMA,
            pltpu.SemaphoreType.DMA,
            pltpu.SemaphoreType.DMA,
            pltpu.SemaphoreType.DMA,
            pltpu.SemaphoreType.DMA,
            pltpu.SemaphoreType.DMA,
            pltpu.SemaphoreType.DMA,
        ],
        compiler_params=pltpu.CompilerParams(
            collective_id=0, has_side_effects=True, vmem_limit_bytes=32 << 20
        ),
    )(
        *(
            pltpu.with_memory_space_constraint(operand, pltpu.HBM)
            for operand in (
                grad_pooled.reshape(batch * tables_all, embed),
                bag_len.T,
                jnp.transpose(lookup_slot, (1, 2, 0)),
                slot_row.reshape(groups, per_peer).T,
                accum,
                weights,
            )
        )
    )
    chunk = min(rows, 128)
    return pl.pallas_call(
        functools.partial(update_kernel, chunk),
        out_shape=(
            jax.ShapeDtypeStruct(weights.shape, F32),
            jax.ShapeDtypeStruct(accum.shape, F32),
        ),
        in_specs=[vmem] * 4,
        out_specs=(anywhere, anywhere),
        scratch_shapes=[
            pltpu.VMEM(weights.shape, F32),
            pltpu.VMEM(accum.shape, F32),
            pltpu.SemaphoreType.DMA((tables * (rows // chunk),)),
            pltpu.SemaphoreType.DMA,
        ],
        compiler_params=pltpu.CompilerParams(vmem_limit_bytes=8 << 20),
    )(held, place, deltas, packed)


def solution(mesh):
    placed = (
        P(("grp", "lane"), None, None),
        P(("grp", "lane"), None),
        P("grp", "lane", None),
        P("grp", "lane", None, None),
        P("lane", "grp", None),
        P("lane", "grp"),
    )
    return jax.shard_map(
        functools.partial(per_device, mesh.shape["grp"], mesh.shape["lane"]),
        mesh=mesh,
        in_specs=placed,
        out_specs=(P("lane", "grp", None), P("lane", "grp")),
        check_vma=False,
    )
```

```python
import functools
import math

import jax
import jax.numpy as jnp
from jax import lax
from jax.experimental import pallas as pl
from jax.experimental.pallas import tpu as pltpu
from jax.sharding import PartitionSpec as P

MESH = pl.DeviceIdType.MESH
LEARN_RATE = 0.3
EPSILON = 1e-06
SIDE = 2
F32 = jnp.float32
BF16 = jnp.bfloat16


def each(count, body):
    if count <= 64:
        for i in range(count):
            body(i)
    else:

        def step(i, carry):
            body(i)
            return carry

        lax.fori_loop(0, count, step, 0)


def iota(shape, dim):
    return lax.broadcasted_iota(jnp.int32, shape, dim)


def kernel(
    groups,
    lanes,
    grad_hbm,
    len_hbm,
    look_hbm,
    slot_hbm,
    accum_hbm,
    weights_hbm,
    packed,
    held,
    place_out,
    delta_out,
    grad_in,
    grad_f32,
    grad_t,
    len_v,
    marks,
    marks_in,
    marks_out,
    slot_v,
    accum_v,
    part_f,
    part,
    recv,
    sums,
    shadow_sums,
    norm_out,
    norm_in,
    load_sem,
    look_sem,
    a_send,
    a_recv,
    b_send,
    b_recv,
    c_send,
    c_recv,
    near_ready,
    far_ready,
    top_ready,
    pair_slot,
    shadow_slot,
    e_send,
    e_recv,
    f_send,
    f_recv,
    g_send,
    g_recv,
):
    devices = groups * lanes
    per_peer, embed = slot_v.shape[0], grad_t.shape[2]
    slots = groups * per_peer
    tables_all, batch = grad_t.shape[0], grad_t.shape[1]
    tables = tables_all // lanes
    depth = marks.shape[2]
    rows = accum_v.shape[1]
    grp = lax.axis_index("grp")
    lane = lax.axis_index("lane")
    me = grp * lanes + lane
    sign = 2 * (grp // (groups // 2)) - 1

    def partial_of(m):
        highs, lows = [], []
        for t in range(tables):
            mark = marks[m, t].astype(F32)
            count = jnp.zeros((slots, batch), F32)
            for j in range(depth):
                count += jnp.where(mark[j : j + 1, :] == number, 1.0, 0.0)
            length = len_v[pl.ds(m * tables + t, 1), :].astype(F32)
            factor = count / length
            high = factor.astype(BF16)
            highs.append(high)
            lows.append((factor - high.astype(F32)).astype(BF16))
        factors = jnp.concatenate(
            [jnp.concatenate(highs, axis=1), jnp.concatenate(lows, axis=1)], axis=0
        )
        values = grad_t[pl.ds(m * tables, tables)].reshape(tables * batch, embed)
        both = jnp.dot(factors, values, preferred_element_type=F32)
        return both[:slots] + both[slots:]

    side = SIDE if groups % (4 * SIDE) == 0 else 1
    depth_all = groups // side
    span = depth_all // 4 * side
    near = groups - span
    near_depth = near // side
    far_depth = depth_all - near_depth
    row, place = grp // side, grp % side
    rows_above, places_above = depth_all - row, side - place
    near_above = jnp.maximum(near_depth - row, 0) * places_above - jnp.where(grp < near, 1, 0)
    far_above = jnp.minimum(rows_above, far_depth) * places_above - jnp.where(grp < near, 0, 1)

    def is_apart(g):
        r, p = g // side, g % side
        return ((r > 0) & (p < side - 1)) | ((r < depth_all - 1) & (p > 0))


    def above(g):
        return (g // side >= row) & (g % side >= place) & (g != grp)

    def below(g):
        return (g // side <= row) & (g % side <= place) & (g != grp)

    half = lanes // 2
    column, core = lane // 2, lane % 2
    leader = core == 1
    widths = embed // 128
    tile = recv.shape[1]
    is_far = grp >= near
    is_top = leader & (grp == groups - 1)
    tells = leader & (grp < near)
    is_shadow = leader & (grp >= near - span) & (grp < near)

    barrier = pltpu.get_barrier_semaphore()
    partner = lane + 1 - 2 * core
    others = [lax.rem(column + d, half) for d in range(1, half)]
    peers = [lane] + [2 * x for x in others] + [2 * x + 1 for x in others] + [partner]

    def signal(semaphore, g, q):
        pl.semaphore_signal(semaphore, inc=1, device_id=(g, q), device_id_type=MESH)

    look_copy = pltpu.make_async_copy(look_hbm, marks_in, look_sem)
    look_copy.start()
    grad_copy = pltpu.make_async_copy(grad_hbm, grad_in, load_sem.at[0])
    weights_copy = pltpu.make_async_copy(weights_hbm, held, look_sem)
    small_copies = [
        pltpu.make_async_copy(len_hbm, len_v, load_sem.at[1]),
        pltpu.make_async_copy(slot_hbm, slot_v, load_sem.at[2]),
    ]
    accum_copy = pltpu.make_async_copy(accum_hbm, accum_v, load_sem.at[2])

    with jax.named_scope("signal_up"):
        for q in peers[1:]:
            signal(barrier, grp, q)

        @pl.loop(grp + 1, groups)
        def _(g):
            @pl.when(above(g))
            def _():
                signal(barrier, g, lane)

        @pl.when(grp < groups - 1)
        def _():
            for x in range(half):

                @pl.when(lane != 2 * x + 1)
                def _():
                    signal(barrier, groups - 1, 2 * x + 1)

    grad_copy.start()
    for copy in small_copies:
        copy.start()

    with jax.named_scope("barrier"):

        @pl.when(is_top)
        def _():
            pl.semaphore_wait(barrier, devices - 1)

        @pl.when(jnp.logical_not(is_top))
        def _():
            pl.semaphore_wait(barrier, lanes - 2 + (row + 1) * (place + 1))

    with jax.named_scope("signal_down"):

        @pl.loop(0, grp)
        def _(g):
            @pl.when(below(g) & is_far)
            def _():
                signal(far_ready, g, lane)

            @pl.when(below(g) & (grp < near))
            def _():
                signal(near_ready, g, lane)

        if side > 1:

            @pl.when(is_top)
            def _():
                @pl.loop(1, groups - 1)
                def _(i):
                    g = groups - 1 - i

                    @pl.when(is_apart(g))
                    def _():
                        for q in range(lanes):
                            signal(top_ready, g, q)

    with jax.named_scope("look_wait"):
        look_copy.wait()

    def marks_for(q):
        piece = marks_in[:, :, pl.ds(pl.multiple_of(q * batch, batch), batch)]
        return piece.astype(F32).astype(marks.dtype)

    for k, q in enumerate(peers[1:]):
        marks_out[k] = marks_for(q)
    for k, q in enumerate(peers[1:], 1):
        pltpu.make_async_remote_copy(
            src_ref=marks_out.at[k - 1],
            dst_ref=marks.at[lane],
            send_sem=a_send,
            recv_sem=a_recv.at[lane],
            device_id=(grp, q),
            device_id_type=MESH,
        ).start()

    with jax.named_scope("grad_wait"):
        grad_copy.wait()
    weights_copy.start()
    with jax.named_scope("grad_turn"):
        for c in range(embed // 128):
            grad_f32[c] = grad_in[:, c * 128 : (c + 1) * 128].astype(F32)
        for t in range(tables_all):
            for c in range(embed // 128):
                grad_t[t, :, c * 128 : (c + 1) * 128] = grad_f32[
                    c, pl.ds(t, batch, stride=tables_all), :
                ].astype(BF16)
    for copy in small_copies:
        copy.wait()
    accum_copy.start()
    pair_copy = pltpu.make_async_remote_copy(
        src_ref=slot_v,
        dst_ref=pair_slot,
        send_sem=e_send,
        recv_sem=e_recv,
        device_id=(grp, lane - core + 1),
        device_id_type=MESH,
    )
    slot_copy = pltpu.make_async_remote_copy(
        src_ref=slot_v,
        dst_ref=shadow_slot.at[core],
        send_sem=f_send,
        recv_sem=f_recv,
        device_id=(jnp.maximum(grp - span, 0), lane - core + 1),
        device_id_type=MESH,
    )

    @pl.when(core == 0)
    def _():
        pair_copy.start()
        pair_slot[...] = jnp.zeros(pair_slot.shape, jnp.int32)

    @pl.when(jnp.logical_not(is_shadow))
    def _():
        shadow_slot[...] = jnp.zeros(shadow_slot.shape, jnp.int32)

    shadow_sums[...] = jnp.zeros(shadow_sums.shape, BF16)

    marks[lane] = marks_for(lane)
    number = iota((slots, batch), 0).astype(F32)

    def take(m):
        total = partial_of(m)
        for h in range(widths):
            part_f[m // 2, pl.ds(m % 2 * widths + h, slots, stride=2 * widths), :] = total[
                :, h * 128 : (h + 1) * 128
            ]

    def marks_from(m, name):
        with jax.named_scope(name):
            pltpu.make_async_copy(marks.at[m], marks.at[m], a_recv.at[m]).wait()

    def settle(x):
        for p in range(groups):
            part[x, p] = part_f[x, p * tile : (p + 1) * tile].astype(BF16)

    def send(p, x):
        pltpu.make_async_remote_copy(
            src_ref=part.at[x, p],
            dst_ref=recv.at[me],
            send_sem=b_send,
            recv_sem=b_recv,
            device_id=(p, 2 * x + 1),
            device_id_type=MESH,
        ).start()

    def send_shadow(p, x):
        pltpu.make_async_remote_copy(
            src_ref=part.at[x, p],
            dst_ref=recv.at[devices + me],
            send_sem=b_send,
            recv_sem=b_recv,
            device_id=(p - span, 2 * x + 1),
            device_id_type=MESH,
        ).start()

    def mine(p, x):
        return leader & (p == grp) & (x == column)

    def each_group(first, last, body):
        if groups <= 16:
            for p in range(first, last):
                body(p)
        else:
            pl.loop(first, last)(body)

    def send_all(first, last, wanted):
        def body(i):
            p = last - 1 + first - i
            for x in range(half):

                @pl.when(wanted(p) & jnp.logical_not(mine(p, x)))
                def _():
                    send(p, x)

        each_group(first, last, body)

    def send_shadows(wanted, columns):
        def body(p):
            for x in columns:
                here = mine(p - span, x)

                @pl.when(wanted(p - span) & jnp.logical_not(here))
                def _():
                    send_shadow(p, x)

                @pl.when(wanted(p - span) & here)
                def _():
                    pltpu.make_async_copy(part.at[x, p], recv.at[devices + me], b_recv).start()

        each_group(near, groups, body)

    def in_line(p):
        return above(p) | below(p) | (p == grp)

    def off_line(p):
        return jnp.logical_not(in_line(p))

    def keep_own():
        @pl.when(leader)
        def _():
            pltpu.make_async_copy(part.at[column, grp], recv.at[me], b_recv).start()

    def near_known():
        with jax.named_scope("near_wait"):

            @pl.when(near_above > 0)
            def _():
                pl.semaphore_wait(near_ready, near_above)

    def far_known():
        with jax.named_scope("far_wait"):

            @pl.when(far_above > 0)
            def _():
                pl.semaphore_wait(far_ready, far_above)

    def rest_known():
        with jax.named_scope("column_wait"):
            pl.semaphore_wait(top_ready, half)

    late = grp >= groups // 2
    take(lane)
    marks_from(partner, "marks_wait1")

    @pl.when(is_far)
    def _():
        slot_copy.start()

    take(partner)
    settle(column)

    @pl.when(late)
    def _():
        near_known()
        far_known()
        pl.when(is_apart(grp))(rest_known)
        send_shadows(lambda p: True, [column])

        def body(p):
            @pl.when(jnp.logical_not(leader & (p == grp)))
            def _():
                send(p, column)

        each_group(0, groups, body)
        keep_own()

    for x in others:
        marks_from(2 * x + 1, "marks_wait2")
        take(2 * x + 1)
    for x in others:
        marks_from(2 * x, "marks_wait3")
        take(2 * x)
    for x in others:
        settle(x)

    @pl.when(late)
    def _():
        for x in others:
            each_group(0, groups, lambda p: send(p, x))
            each_group(near, groups, lambda p: send_shadow(p, x))

    @pl.when(jnp.logical_not(late))
    def _():
        near_known()
        send_shadows(in_line, range(half))
        send_all(0, near, in_line)
        keep_own()
        far_known()
        send_all(near, groups, in_line)

        @pl.when(is_apart(grp))
        def _():
            rest_known()
            send_shadows(off_line, range(half))
            send_all(0, groups, off_line)

    with jax.named_scope("sent"):
        pass

    two = 2 * slots
    which = iota((two, groups), 0)
    span_of = tables * rows

    def named_rows(low, high):
        low, high = low.astype(F32), high.astype(F32)
        pick = jnp.zeros((two, groups), F32)
        for k in range(per_peer):
            pick = jnp.where(which % (2 * per_peer) == 2 * k, low[k : k + 1, :], pick)
            pick = jnp.where(which % (2 * per_peer) == 2 * k + 1, high[k : k + 1, :], pick)
        pick = jnp.where(which // (2 * per_peer) == iota((two, groups), 1), pick, 0.0)
        return jnp.sum(pick, axis=1, keepdims=True)

    @pl.when(leader)
    def _():
        pair_copy.wait_recv()

    @pl.when(is_shadow)
    def _():
        pltpu.make_async_copy(shadow_slot, shadow_slot, f_recv).wait()

    own_slot, other_slot = slot_v[...], pair_slot[...] + span_of
    target_col = jnp.concatenate(
        [
            named_rows(
                jnp.where(leader, other_slot, own_slot), jnp.where(leader, own_slot, other_slot)
            ),
            named_rows(shadow_slot[0] + 2 * span_of, shadow_slot[1] + 3 * span_of),
        ],
        axis=0,
    )
    i_id, j_id = iota((2 * two, 2 * two), 0), iota((2 * two, 2 * two), 1)
    target_row = jnp.sum(jnp.where(i_id == j_id, target_col, 0.0), axis=0, keepdims=True)
    same = target_col == target_row
    first_col = jnp.sum(jnp.where(same & (j_id < i_id), 1.0, 0.0), axis=1, keepdims=True) == 0.0
    first_row = jnp.sum(jnp.where(same & (i_id < j_id), 1.0, 0.0), axis=0, keepdims=True) == 0.0
    is_own = (target_row < span_of) & first_row
    place_row = jnp.where(is_own, target_row, -1.0)[:, :two]
    place_row = jnp.concatenate([place_row, place_row], axis=1)
    for r in range(0, span_of, 128):
        row_id = (iota((128, 1), 0) + r).astype(F32)
        place_out[r : r + 128] = jnp.where(row_id == place_row, 1.0, 0.0).astype(BF16)
    wide = (2 * two, widths * 2 * two)
    wide_i, wide_j = iota(wide, 0), iota(wide, 1)
    spread_row = jnp.sum(
        jnp.where(wide_i == wide_j // widths, target_col, 0.0), axis=0, keepdims=True
    )
    picks = [
        jnp.where((target_col == spread_row) & (wide_j % widths == h), 1.0, 0.0).astype(BF16)
        for h in range(widths)
    ]

    accum_copy.wait()
    hits = []
    accum_col = jnp.zeros((two, 1), F32)
    for t in range(tables):
        hit = target_col[:two] == (iota((two, rows), 1) + t * rows).astype(F32)
        hits.append(hit)
        accum_col += jnp.sum(
            jnp.where(hit, accum_v[t : t + 1, :], 0.0), axis=1, keepdims=True
        )

    def gather(base):
        group_sums = []
        for g in range(groups):
            group_sum = recv[base + g * lanes].astype(F32)
            for q in range(1, lanes):
                group_sum += recv[base + g * lanes + q].astype(F32)
            group_sums.append(group_sum)
        return jnp.concatenate(group_sums, axis=0).astype(BF16)

    sums_copy = pltpu.make_async_remote_copy(
        src_ref=sums,
        dst_ref=sums,
        send_sem=g_send,
        recv_sem=g_recv,
        device_id=(grp, lane - core),
        device_id_type=MESH,
    )

    with jax.named_scope("sums_wait"):

        @pl.when(is_shadow)
        def _():
            pltpu.make_async_copy(recv, recv, b_recv).wait()
            shadow_sums[...] = gather(devices)

        @pl.when(leader & jnp.logical_not(is_shadow))
        def _():
            came = recv.at[pl.ds(0, devices)]
            pltpu.make_async_copy(came, came, b_recv).wait()

        @pl.when(leader)
        def _():
            sums[...] = gather(0)
            sums_copy.start()

        @pl.when(core == 0)
        def _():
            sums_copy.wait_recv()

    all_sums = jnp.concatenate([sums[...], shadow_sums[...]], axis=0)
    pieces = [jnp.dot(pick, all_sums, preferred_element_type=F32) for pick in picks]
    squares = sum(piece * piece for piece in pieces)
    norm_out[...] = jnp.sum(jnp.where(first_col, squares, 0.0), axis=0, keepdims=True)

    def tell(far):
        pltpu.make_async_remote_copy(
            src_ref=norm_out,
            dst_ref=norm_in.at[grp * half + column],
            send_sem=c_send,
            recv_sem=c_recv,
            device_id=(far // lanes, far % lanes),
            device_id_type=MESH,
        ).start()

    @pl.when(tells)
    def _():
        each(devices - 1, lambda i: tell(jnp.where(i < me, i, i + 1)))
        pltpu.make_async_copy(norm_out, norm_in.at[grp * half + column], c_recv).start()

    grads = jnp.concatenate([piece[:two] for piece in pieces], axis=1)
    square_col = jnp.sum(squares[:two], axis=1, keepdims=True) * (1.0 / embed)
    square_first = jnp.where(first_col[:two], square_col, 0.0)
    square_rows = [
        jnp.sum(jnp.where(hit, square_first, 0.0), axis=0, keepdims=True) for hit in hits
    ]
    pltpu.make_async_copy(marks_out, marks_out, a_send).wait()

    def sent(count):
        piece = recv.at[pl.ds(0, count)]
        pltpu.make_async_copy(piece, piece, b_send).wait()

    total_sent = (groups + span) * half
    if span > 0:
        pl.when(is_shadow)(lambda: sent(total_sent - 2))
    pl.when(leader & jnp.logical_not(is_shadow))(lambda: sent(total_sent - 1))
    pl.when(core == 0)(lambda: sent(total_sent))

    @pl.when(is_far)
    def _():
        slot_copy.wait_send()

    @pl.when(core == 0)
    def _():
        pair_copy.wait_send()

    @pl.when(leader)
    def _():
        sums_copy.wait_send()

    with jax.named_scope("norm_wait"):
        told = norm_in.at[pl.ds(0, near * half)]
        pltpu.make_async_copy(told, told, c_recv).wait()
    weights_copy.wait()
    norm_total = jnp.sum(jnp.sum(norm_in[: near * half], axis=0), axis=1, keepdims=True)
    clip_limit = 0.25 * devices * slots * embed
    clip_square = clip_limit / jnp.maximum(norm_total, clip_limit)
    for t in range(tables):
        packed[t : t + 1, :] = accum_v[t : t + 1, :] + clip_square * square_rows[t]
    new_accum_col = accum_col + clip_square * square_col
    rate = LEARN_RATE * jnp.sqrt(clip_square) / (jnp.sqrt(new_accum_col) + EPSILON)
    delta = rate * grads
    high = delta.astype(BF16)
    delta_out[:two] = high
    delta_out[two:] = (delta - high.astype(F32)).astype(BF16)

    @pl.when(tells)
    def _():
        told = norm_in.at[pl.ds(0, devices - 1)]
        pltpu.make_async_copy(told, told, c_send).wait()


def update_kernel(chunk, weights, place, deltas, packed, wout, aout, held, accum, sems, accum_sem):
    tables, rows = weights.shape[0], weights.shape[1]
    copies = []
    for t in range(tables):
        for c in range(0, rows, chunk):
            held[t, c : c + chunk] = weights[t, c : c + chunk] - jnp.dot(
                place[t * rows + c : t * rows + c + chunk],
                deltas[...],
                preferred_element_type=F32,
            )
            copies.append(
                pltpu.make_async_copy(
                    held.at[t, pl.ds(c, chunk)],
                    wout.at[t, pl.ds(c, chunk)],
                    sems,
                )
            )
            copies[-1].start()
    accum[...] = packed[...]
    accum_copy = pltpu.make_async_copy(accum, aout, accum_sem)
    accum_copy.start()
    pltpu.make_async_copy(held, wout, sems).wait()
    accum_copy.wait()


def per_device(groups, lanes, grad_pooled, bag_len, lookup_slot, slot_row, weights, accum):
    batch, tables_all, embed = grad_pooled.shape
    samples, tables, depth = lookup_slot.shape
    rows = accum.shape[1]
    per_peer = slot_row.shape[3]
    devices = groups * lanes
    slots = groups * per_peer
    mark_type = BF16 if slots <= 256 else F32
    half = lanes // 2
    tile = 2 * per_peer * (embed // 128)
    anywhere = pl.BlockSpec(memory_space=pl.ANY)
    vmem = pl.BlockSpec(memory_space=pltpu.VMEM)
    packed, held, place, deltas = pl.pallas_call(
        functools.partial(kernel, groups, lanes),
        out_shape=(
            jax.ShapeDtypeStruct(accum.shape, F32),
            jax.ShapeDtypeStruct(weights.shape, F32),
            jax.ShapeDtypeStruct((tables * rows, 4 * slots), BF16),
            jax.ShapeDtypeStruct((4 * slots, embed), BF16),
        ),
        in_specs=[pl.BlockSpec(memory_space=pltpu.HBM)] * 6,
        out_specs=(vmem,) * 4,
        cost_estimate=pl.CostEstimate(
            flops=8 * slots * batch * tables_all * embed,
            bytes_accessed=32 * batch * tables_all * embed,
            transcendentals=0,
        ),
        scratch_shapes=[
            pltpu.VMEM((batch * tables_all, embed), BF16),
            pltpu.VMEM((embed // 128, batch * tables_all, 128), F32),
            pltpu.VMEM((tables_all, batch, embed), BF16),
            pltpu.VMEM((tables_all, batch), jnp.int32),
            pltpu.VMEM((lanes, tables, depth, batch), mark_type),
            pltpu.VMEM((tables, depth, samples), jnp.int32),
            pltpu.VMEM((lanes - 1, tables, depth, batch), mark_type),
            pltpu.VMEM((per_peer, groups), jnp.int32),
            pltpu.VMEM((tables, rows), F32),
            pltpu.VMEM((half, groups * tile, 128), F32),
            pltpu.VMEM((half, groups, tile, 128), BF16),
            pltpu.VMEM((2 * devices, tile, 128), BF16),
            pltpu.VMEM((groups * tile, 128), BF16),
            pltpu.VMEM((groups * tile, 128), BF16),
            pltpu.VMEM((1, 128), F32),
            pltpu.VMEM((devices, 1, 128), F32),
            pltpu.SemaphoreType.DMA((3,)),
            pltpu.SemaphoreType.DMA,
            pltpu.SemaphoreType.DMA,
            pltpu.SemaphoreType.DMA((lanes,)),
            pltpu.SemaphoreType.DMA,
            pltpu.SemaphoreType.DMA,
            pltpu.SemaphoreType.DMA,
            pltpu.SemaphoreType.DMA,
            pltpu.SemaphoreType.REGULAR,
            pltpu.SemaphoreType.REGULAR,
            pltpu.SemaphoreType.REGULAR,
            pltpu.VMEM((per_peer, groups), jnp.int32),
            pltpu.VMEM((2, per_peer, groups), jnp.int32),
            pltpu.SemaphoreType.DMA,
            pltpu.SemaphoreType.DMA,
            pltpu.SemaphoreType.DMA,
            pltpu.SemaphoreType.DMA,
            pltpu.SemaphoreType.DMA,
            pltpu.SemaphoreType.DMA,
        ],
        compiler_params=pltpu.CompilerParams(
            collective_id=0, has_side_effects=True, vmem_limit_bytes=32 << 20
        ),
    )(
        *(
            pltpu.with_memory_space_constraint(operand, pltpu.HBM)
            for operand in (
                grad_pooled.reshape(batch * tables_all, embed),
                bag_len.T,
                jnp.transpose(lookup_slot, (1, 2, 0)),
                slot_row.reshape(groups, per_peer).T,
                accum,
                weights,
            )
        )
    )
    chunk = min(rows, 128)
    return pl.pallas_call(
        functools.partial(update_kernel, chunk),
        out_shape=(
            jax.ShapeDtypeStruct(weights.shape, F32),
            jax.ShapeDtypeStruct(accum.shape, F32),
        ),
        in_specs=[vmem] * 4,
        out_specs=(anywhere, anywhere),
        scratch_shapes=[
            pltpu.VMEM(weights.shape, F32),
            pltpu.VMEM(accum.shape, F32),
            pltpu.SemaphoreType.DMA,
            pltpu.SemaphoreType.DMA,
        ],
        compiler_params=pltpu.CompilerParams(vmem_limit_bytes=8 << 20),
    )(held, place, deltas, packed)


def solution(mesh):
    placed = (
        P(("grp", "lane"), None, None),
        P(("grp", "lane"), None),
        P("grp", "lane", None),
        P("grp", "lane", None, None),
        P("lane", "grp", None),
        P("lane", "grp"),
    )
    return jax.shard_map(
        functools.partial(per_device, mesh.shape["grp"], mesh.shape["lane"]),
        mesh=mesh,
        in_specs=placed,
        out_specs=(P("lane", "grp", None), P("lane", "grp")),
        check_vma=False,
    )
```

```python
import functools
import math

import jax
import jax.numpy as jnp
from jax import lax
from jax.experimental import pallas as pl
from jax.experimental.pallas import tpu as pltpu
from jax.sharding import PartitionSpec as P

MESH = pl.DeviceIdType.MESH
LEARN_RATE = 0.3
EPSILON = 1e-06
SIDE = 2
F32 = jnp.float32
BF16 = jnp.bfloat16


def each(count, body):
    if count <= 64:
        for i in range(count):
            body(i)
    else:

        def step(i, carry):
            body(i)
            return carry

        lax.fori_loop(0, count, step, 0)


def iota(shape, dim):
    return lax.broadcasted_iota(jnp.int32, shape, dim)


def kernel(
    groups,
    lanes,
    grad_hbm,
    len_hbm,
    look_hbm,
    slot_hbm,
    accum_hbm,
    weights_hbm,
    packed,
    held,
    place_out,
    delta_out,
    grad_in,
    grad_f32,
    grad_t,
    len_v,
    marks,
    marks_in,
    marks_out,
    slot_v,
    accum_v,
    part_f,
    part,
    recv,
    sums,
    shadow_sums,
    norm_out,
    norm_in,
    load_sem,
    look_sem,
    a_send,
    a_recv,
    b_send,
    b_recv,
    c_send,
    c_recv,
    near_ready,
    far_ready,
    top_ready,
    pair_slot,
    shadow_slot,
    e_send,
    e_recv,
    f_send,
    f_recv,
):
    devices = groups * lanes
    per_peer, embed = slot_v.shape[0], grad_t.shape[2]
    slots = groups * per_peer
    tables_all, batch = grad_t.shape[0], grad_t.shape[1]
    tables = tables_all // lanes
    depth = marks.shape[2]
    rows = accum_v.shape[1]
    grp = lax.axis_index("grp")
    lane = lax.axis_index("lane")
    me = grp * lanes + lane
    sign = 2 * (grp // (groups // 2)) - 1

    def partial_of(m):
        highs, lows = [], []
        for t in range(tables):
            mark = marks[m, t].astype(F32)
            count = jnp.zeros((slots, batch), F32)
            for j in range(depth):
                count += jnp.where(mark[j : j + 1, :] == number, 1.0, 0.0)
            length = len_v[pl.ds(m * tables + t, 1), :].astype(F32)
            factor = count / length
            high = factor.astype(BF16)
            highs.append(high)
            lows.append((factor - high.astype(F32)).astype(BF16))
        factors = jnp.concatenate(
            [jnp.concatenate(highs, axis=1), jnp.concatenate(lows, axis=1)], axis=0
        )
        values = grad_t[pl.ds(m * tables, tables)].reshape(tables * batch, embed)
        both = jnp.dot(factors, values, preferred_element_type=F32)
        return both[:slots] + both[slots:]

    side = SIDE if groups % (4 * SIDE) == 0 else 1
    depth_all = groups // side
    span = depth_all // 4 * side
    near = groups - span
    near_depth = near // side
    far_depth = depth_all - near_depth
    row, place = grp // side, grp % side
    rows_above, places_above = depth_all - row, side - place
    near_above = jnp.maximum(near_depth - row, 0) * places_above - jnp.where(grp < near, 1, 0)
    far_above = jnp.minimum(rows_above, far_depth) * places_above - jnp.where(grp < near, 0, 1)

    def is_apart(g):
        r, p = g // side, g % side
        return ((r > 0) & (p < side - 1)) | ((r < depth_all - 1) & (p > 0))


    def above(g):
        return (g // side >= row) & (g % side >= place) & (g != grp)

    def below(g):
        return (g // side <= row) & (g % side <= place) & (g != grp)

    half = lanes // 2
    column, core = lane // 2, lane % 2
    leader = core == 1
    widths = embed // 128
    tile = recv.shape[1]
    is_far = grp >= near
    is_top = leader & (grp == groups - 1)
    tells = leader & (grp < near)
    is_shadow = leader & (grp >= near - span) & (grp < near)

    barrier = pltpu.get_barrier_semaphore()
    partner = lane + 1 - 2 * core
    others = [lax.rem(column + d, half) for d in range(1, half)]
    peers = [lane] + [2 * x for x in others] + [2 * x + 1 for x in others] + [partner]

    def signal(semaphore, g, q):
        pl.semaphore_signal(semaphore, inc=1, device_id=(g, q), device_id_type=MESH)

    look_copy = pltpu.make_async_copy(look_hbm, marks_in, look_sem)
    look_copy.start()
    grad_copy = pltpu.make_async_copy(grad_hbm, grad_in, load_sem.at[0])
    weights_copy = pltpu.make_async_copy(weights_hbm, held, look_sem)
    small_copies = [
        pltpu.make_async_copy(len_hbm, len_v, load_sem.at[1]),
        pltpu.make_async_copy(slot_hbm, slot_v, load_sem.at[2]),
    ]
    accum_copy = pltpu.make_async_copy(accum_hbm, accum_v, load_sem.at[2])

    with jax.named_scope("signal_up"):
        for q in peers[1:]:
            signal(barrier, grp, q)

        @pl.loop(grp + 1, groups)
        def _(g):
            @pl.when(above(g))
            def _():
                signal(barrier, g, lane)

        @pl.when(grp < groups - 1)
        def _():
            for x in range(half):

                @pl.when(lane != 2 * x + 1)
                def _():
                    signal(barrier, groups - 1, 2 * x + 1)

    grad_copy.start()
    for copy in small_copies:
        copy.start()

    with jax.named_scope("barrier"):

        @pl.when(is_top)
        def _():
            pl.semaphore_wait(barrier, devices - 1)

        @pl.when(jnp.logical_not(is_top))
        def _():
            pl.semaphore_wait(barrier, lanes - 2 + (row + 1) * (place + 1))

    with jax.named_scope("signal_down"):

        @pl.loop(0, grp)
        def _(g):
            @pl.when(below(g) & is_far)
            def _():
                signal(far_ready, g, lane)

            @pl.when(below(g) & (grp < near))
            def _():
                signal(near_ready, g, lane)

        if side > 1:

            @pl.when(is_top)
            def _():
                @pl.loop(1, groups - 1)
                def _(i):
                    g = groups - 1 - i

                    @pl.when(is_apart(g))
                    def _():
                        for q in range(lanes):
                            signal(top_ready, g, q)

    with jax.named_scope("look_wait"):
        look_copy.wait()

    def marks_for(q):
        piece = marks_in[:, :, pl.ds(pl.multiple_of(q * batch, batch), batch)]
        return piece.astype(F32).astype(marks.dtype)

    for k, q in enumerate(peers[1:]):
        marks_out[k] = marks_for(q)
    for k, q in enumerate(peers[1:], 1):
        pltpu.make_async_remote_copy(
            src_ref=marks_out.at[k - 1],
            dst_ref=marks.at[lane],
            send_sem=a_send,
            recv_sem=a_recv.at[lax.rem(lane - q + lanes, lanes) - 1],
            device_id=(grp, q),
            device_id_type=MESH,
        ).start()

    with jax.named_scope("grad_wait"):
        grad_copy.wait()
    weights_copy.start()
    with jax.named_scope("grad_turn"):
        for c in range(embed // 128):
            grad_f32[c] = grad_in[:, c * 128 : (c + 1) * 128].astype(F32)
        for t in range(tables_all):
            for c in range(embed // 128):
                grad_t[t, :, c * 128 : (c + 1) * 128] = grad_f32[
                    c, pl.ds(t, batch, stride=tables_all), :
                ].astype(BF16)
    for copy in small_copies:
        copy.wait()
    accum_copy.start()
    pair_copy = pltpu.make_async_remote_copy(
        src_ref=slot_v,
        dst_ref=pair_slot,
        send_sem=e_send,
        recv_sem=e_recv,
        device_id=(grp, lane - core + 1),
        device_id_type=MESH,
    )
    slot_copy = pltpu.make_async_remote_copy(
        src_ref=slot_v,
        dst_ref=shadow_slot.at[core],
        send_sem=f_send,
        recv_sem=f_recv,
        device_id=(jnp.maximum(grp - span, 0), lane - core + 1),
        device_id_type=MESH,
    )

    @pl.when(core == 0)
    def _():
        pair_copy.start()
        pair_slot[...] = jnp.zeros(pair_slot.shape, jnp.int32)

    @pl.when(jnp.logical_not(is_shadow))
    def _():
        shadow_slot[...] = jnp.zeros(shadow_slot.shape, jnp.int32)

    shadow_sums[...] = jnp.zeros(shadow_sums.shape, BF16)

    marks[lane] = marks_for(lane)
    number = iota((slots, batch), 0).astype(F32)

    def take(m):
        total = partial_of(m)
        for h in range(widths):
            part_f[m // 2, pl.ds(m % 2 * widths + h, slots, stride=2 * widths), :] = total[
                :, h * 128 : (h + 1) * 128
            ]

    def marks_from(m, name):
        with jax.named_scope(name):
            slot = lax.rem(m - lane + lanes, lanes) - 1
            pltpu.make_async_copy(marks.at[m], marks.at[m], a_recv.at[slot]).wait()

    def settle(x):
        for p in range(groups):
            part[x, p] = part_f[x, p * tile : (p + 1) * tile].astype(BF16)

    def send(p, x):
        pltpu.make_async_remote_copy(
            src_ref=part.at[x, p],
            dst_ref=recv.at[me],
            send_sem=b_send,
            recv_sem=b_recv,
            device_id=(p, 2 * x + 1),
            device_id_type=MESH,
        ).start()

    def send_shadow(p, x):
        pltpu.make_async_remote_copy(
            src_ref=part.at[x, p],
            dst_ref=recv.at[devices + me],
            send_sem=b_send,
            recv_sem=b_recv,
            device_id=(p - span, 2 * x + 1),
            device_id_type=MESH,
        ).start()

    def mine(p, x):
        return leader & (p == grp) & (x == column)

    def each_group(first, last, body):
        if groups <= 16:
            for p in range(first, last):
                body(p)
        else:
            pl.loop(first, last)(body)

    def send_all(first, last, wanted):
        def body(i):
            p = last - 1 + first - i
            for x in range(half):

                @pl.when(wanted(p) & jnp.logical_not(mine(p, x)))
                def _():
                    send(p, x)

        each_group(first, last, body)

    def send_shadows(wanted, columns):
        def body(p):
            for x in columns:
                here = mine(p - span, x)

                @pl.when(wanted(p - span) & jnp.logical_not(here))
                def _():
                    send_shadow(p, x)

                @pl.when(wanted(p - span) & here)
                def _():
                    pltpu.make_async_copy(part.at[x, p], recv.at[devices + me], b_recv).start()

        each_group(near, groups, body)

    def in_line(p):
        return above(p) | below(p) | (p == grp)

    def off_line(p):
        return jnp.logical_not(in_line(p))

    def keep_own():
        @pl.when(leader)
        def _():
            pltpu.make_async_copy(part.at[column, grp], recv.at[me], b_recv).start()

    def near_known():
        with jax.named_scope("near_wait"):

            @pl.when(near_above > 0)
            def _():
                pl.semaphore_wait(near_ready, near_above)

    def far_known():
        with jax.named_scope("far_wait"):

            @pl.when(far_above > 0)
            def _():
                pl.semaphore_wait(far_ready, far_above)

    def rest_known():
        with jax.named_scope("column_wait"):
            pl.semaphore_wait(top_ready, half)

    late = grp >= groups // 2
    take(lane)
    marks_from(partner, "marks_wait1")

    @pl.when(is_far)
    def _():
        slot_copy.start()

    take(partner)
    settle(column)

    @pl.when(late)
    def _():
        near_known()
        far_known()
        pl.when(is_apart(grp))(rest_known)
        send_shadows(lambda p: True, [column])

        def body(p):
            @pl.when(jnp.logical_not(leader & (p == grp)))
            def _():
                send(p, column)

        each_group(0, groups, body)
        keep_own()

    for x in others:
        marks_from(2 * x + 1, "marks_wait2")
        take(2 * x + 1)
    for x in others:
        marks_from(2 * x, "marks_wait3")
        take(2 * x)
    for x in others:
        settle(x)

    @pl.when(late)
    def _():
        for x in others:
            each_group(0, groups, lambda p: send(p, x))
            each_group(near, groups, lambda p: send_shadow(p, x))

    @pl.when(jnp.logical_not(late))
    def _():
        near_known()
        send_shadows(in_line, range(half))
        send_all(0, near, in_line)
        keep_own()
        far_known()
        send_all(near, groups, in_line)

        @pl.when(is_apart(grp))
        def _():
            rest_known()
            send_shadows(off_line, range(half))
            send_all(0, groups, off_line)

    with jax.named_scope("sent"):
        pass

    two = 2 * slots
    which = iota((two, groups), 0)
    span_of = tables * rows

    def named_rows(low, high):
        low, high = low.astype(F32), high.astype(F32)
        pick = jnp.zeros((two, groups), F32)
        for k in range(per_peer):
            pick = jnp.where(which % (2 * per_peer) == 2 * k, low[k : k + 1, :], pick)
            pick = jnp.where(which % (2 * per_peer) == 2 * k + 1, high[k : k + 1, :], pick)
        pick = jnp.where(which // (2 * per_peer) == iota((two, groups), 1), pick, 0.0)
        return jnp.sum(pick, axis=1, keepdims=True)

    @pl.when(leader)
    def _():
        pair_copy.wait_recv()

    @pl.when(is_shadow)
    def _():
        pltpu.make_async_copy(shadow_slot, shadow_slot, f_recv).wait()

    own_slot, other_slot = slot_v[...], pair_slot[...] + span_of
    target_col = jnp.concatenate(
        [
            named_rows(
                jnp.where(leader, other_slot, own_slot), jnp.where(leader, own_slot, other_slot)
            ),
            named_rows(shadow_slot[0] + 2 * span_of, shadow_slot[1] + 3 * span_of),
        ],
        axis=0,
    )
    i_id, j_id = iota((2 * two, 2 * two), 0), iota((2 * two, 2 * two), 1)
    target_row = jnp.sum(jnp.where(i_id == j_id, target_col, 0.0), axis=0, keepdims=True)
    same = target_col == target_row
    first_col = jnp.sum(jnp.where(same & (j_id < i_id), 1.0, 0.0), axis=1, keepdims=True) == 0.0
    first_row = jnp.sum(jnp.where(same & (i_id < j_id), 1.0, 0.0), axis=0, keepdims=True) == 0.0
    is_own = (target_row < span_of) & first_row
    place_row = jnp.where(is_own, target_row, -1.0)[:, :two]
    place_row = jnp.concatenate([place_row, place_row], axis=1)
    for r in range(0, span_of, 128):
        row_id = (iota((128, 1), 0) + r).astype(F32)
        place_out[r : r + 128] = jnp.where(row_id == place_row, 1.0, 0.0).astype(BF16)
    wide = (2 * two, widths * 2 * two)
    wide_i, wide_j = iota(wide, 0), iota(wide, 1)
    spread_row = jnp.sum(
        jnp.where(wide_i == wide_j // widths, target_col, 0.0), axis=0, keepdims=True
    )
    picks = [
        jnp.where((target_col == spread_row) & (wide_j % widths == h), 1.0, 0.0).astype(BF16)
        for h in range(widths)
    ]

    accum_copy.wait()
    hits = []
    accum_col = jnp.zeros((two, 1), F32)
    for t in range(tables):
        hit = target_col[:two] == (iota((two, rows), 1) + t * rows).astype(F32)
        hits.append(hit)
        accum_col += jnp.sum(
            jnp.where(hit, accum_v[t : t + 1, :], 0.0), axis=1, keepdims=True
        )

    def gather(base):
        group_sums = []
        for g in range(groups):
            group_sum = recv[base + g * lanes].astype(F32)
            for q in range(1, lanes):
                group_sum += recv[base + g * lanes + q].astype(F32)
            group_sums.append(group_sum)
        return jnp.concatenate(group_sums, axis=0).astype(BF16)

    sums_copy = pltpu.make_async_remote_copy(
        src_ref=sums,
        dst_ref=sums,
        send_sem=e_send,
        recv_sem=e_recv,
        device_id=(grp, lane - core),
        device_id_type=MESH,
    )

    with jax.named_scope("sums_wait"):

        @pl.when(is_shadow)
        def _():
            pltpu.make_async_copy(recv, recv, b_recv).wait()
            shadow_sums[...] = gather(devices)

        @pl.when(leader & jnp.logical_not(is_shadow))
        def _():
            came = recv.at[pl.ds(0, devices)]
            pltpu.make_async_copy(came, came, b_recv).wait()

        @pl.when(leader)
        def _():
            sums[...] = gather(0)
            sums_copy.start()

        @pl.when(core == 0)
        def _():
            sums_copy.wait_recv()

    all_sums = jnp.concatenate([sums[...], shadow_sums[...]], axis=0)
    pieces = [jnp.dot(pick, all_sums, preferred_element_type=F32) for pick in picks]
    squares = sum(piece * piece for piece in pieces)
    norm_out[...] = jnp.sum(jnp.where(first_col, squares, 0.0), axis=0, keepdims=True)

    def tell(far):
        pltpu.make_async_remote_copy(
            src_ref=norm_out,
            dst_ref=norm_in.at[grp * half + column],
            send_sem=c_send,
            recv_sem=c_recv,
            device_id=(far // lanes, far % lanes),
            device_id_type=MESH,
        ).start()

    @pl.when(tells)
    def _():
        each(devices - 1, lambda i: tell(jnp.where(i < me, i, i + 1)))
        pltpu.make_async_copy(norm_out, norm_in.at[grp * half + column], c_recv).start()

    grads = jnp.concatenate([piece[:two] for piece in pieces], axis=1)
    square_col = jnp.sum(squares[:two], axis=1, keepdims=True) * (1.0 / embed)
    square_first = jnp.where(first_col[:two], square_col, 0.0)
    square_rows = [
        jnp.sum(jnp.where(hit, square_first, 0.0), axis=0, keepdims=True) for hit in hits
    ]
    pltpu.make_async_copy(marks_out, marks_out, a_send).wait()

    def sent(count):
        piece = recv.at[pl.ds(0, count)]
        pltpu.make_async_copy(piece, piece, b_send).wait()

    total_sent = (groups + span) * half
    if span > 0:
        pl.when(is_shadow)(lambda: sent(total_sent - 2))
    pl.when(leader & jnp.logical_not(is_shadow))(lambda: sent(total_sent - 1))
    pl.when(core == 0)(lambda: sent(total_sent))

    @pl.when(is_far)
    def _():
        slot_copy.wait_send()

    @pl.when(core == 0)
    def _():
        pair_copy.wait_send()

    @pl.when(leader)
    def _():
        sums_copy.wait_send()

    with jax.named_scope("norm_wait"):
        told = norm_in.at[pl.ds(0, near * half)]
        pltpu.make_async_copy(told, told, c_recv).wait()
    weights_copy.wait()
    norm_total = jnp.sum(jnp.sum(norm_in[: near * half], axis=0), axis=1, keepdims=True)
    clip_limit = 0.25 * devices * slots * embed
    clip_square = clip_limit / jnp.maximum(norm_total, clip_limit)
    for t in range(tables):
        packed[t : t + 1, :] = accum_v[t : t + 1, :] + clip_square * square_rows[t]
    new_accum_col = accum_col + clip_square * square_col
    rate = LEARN_RATE * jnp.sqrt(clip_square) / (jnp.sqrt(new_accum_col) + EPSILON)
    delta = rate * grads
    high = delta.astype(BF16)
    delta_out[:two] = high
    delta_out[two:] = (delta - high.astype(F32)).astype(BF16)

    @pl.when(tells)
    def _():
        told = norm_in.at[pl.ds(0, devices - 1)]
        pltpu.make_async_copy(told, told, c_send).wait()


def update_kernel(chunk, weights, place, deltas, packed, wout, aout, held, accum, sems, accum_sem):
    tables, rows = weights.shape[0], weights.shape[1]
    copies = []
    for t in range(tables):
        for c in range(0, rows, chunk):
            held[t, c : c + chunk] = weights[t, c : c + chunk] - jnp.dot(
                place[t * rows + c : t * rows + c + chunk],
                deltas[...],
                preferred_element_type=F32,
            )
            copies.append(
                pltpu.make_async_copy(
                    held.at[t, pl.ds(c, chunk)],
                    wout.at[t, pl.ds(c, chunk)],
                    sems,
                )
            )
            copies[-1].start()
    accum[...] = packed[...]
    accum_copy = pltpu.make_async_copy(accum, aout, accum_sem)
    accum_copy.start()
    pltpu.make_async_copy(held, wout, sems).wait()
    accum_copy.wait()


def per_device(groups, lanes, grad_pooled, bag_len, lookup_slot, slot_row, weights, accum):
    batch, tables_all, embed = grad_pooled.shape
    samples, tables, depth = lookup_slot.shape
    rows = accum.shape[1]
    per_peer = slot_row.shape[3]
    devices = groups * lanes
    slots = groups * per_peer
    mark_type = BF16 if slots <= 256 else F32
    half = lanes // 2
    tile = 2 * per_peer * (embed // 128)
    anywhere = pl.BlockSpec(memory_space=pl.ANY)
    vmem = pl.BlockSpec(memory_space=pltpu.VMEM)
    packed, held, place, deltas = pl.pallas_call(
        functools.partial(kernel, groups, lanes),
        out_shape=(
            jax.ShapeDtypeStruct(accum.shape, F32),
            jax.ShapeDtypeStruct(weights.shape, F32),
            jax.ShapeDtypeStruct((tables * rows, 4 * slots), BF16),
            jax.ShapeDtypeStruct((4 * slots, embed), BF16),
        ),
        in_specs=[pl.BlockSpec(memory_space=pltpu.HBM)] * 6,
        out_specs=(vmem,) * 4,
        cost_estimate=pl.CostEstimate(
            flops=8 * slots * batch * tables_all * embed,
            bytes_accessed=32 * batch * tables_all * embed,
            transcendentals=0,
        ),
        scratch_shapes=[
            pltpu.VMEM((batch * tables_all, embed), BF16),
            pltpu.VMEM((embed // 128, batch * tables_all, 128), F32),
            pltpu.VMEM((tables_all, batch, embed), BF16),
            pltpu.VMEM((tables_all, batch), jnp.int32),
            pltpu.VMEM((lanes, tables, depth, batch), mark_type),
            pltpu.VMEM((tables, depth, samples), jnp.int32),
            pltpu.VMEM((lanes - 1, tables, depth, batch), mark_type),
            pltpu.VMEM((per_peer, groups), jnp.int32),
            pltpu.VMEM((tables, rows), F32),
            pltpu.VMEM((half, groups * tile, 128), F32),
            pltpu.VMEM((half, groups, tile, 128), BF16),
            pltpu.VMEM((2 * devices, tile, 128), BF16),
            pltpu.VMEM((groups * tile, 128), BF16),
            pltpu.VMEM((groups * tile, 128), BF16),
            pltpu.VMEM((1, 128), F32),
            pltpu.VMEM((devices, 1, 128), F32),
            pltpu.SemaphoreType.DMA((3,)),
            pltpu.SemaphoreType.DMA,
            pltpu.SemaphoreType.DMA,
            pltpu.SemaphoreType.DMA((lanes - 1,)),
            pltpu.SemaphoreType.DMA,
            pltpu.SemaphoreType.DMA,
            pltpu.SemaphoreType.DMA,
            pltpu.SemaphoreType.DMA,
            pltpu.SemaphoreType.REGULAR,
            pltpu.SemaphoreType.REGULAR,
            pltpu.SemaphoreType.REGULAR,
            pltpu.VMEM((per_peer, groups), jnp.int32),
            pltpu.VMEM((2, per_peer, groups), jnp.int32),
            pltpu.SemaphoreType.DMA,
            pltpu.SemaphoreType.DMA,
            pltpu.SemaphoreType.DMA,
            pltpu.SemaphoreType.DMA,
        ],
        compiler_params=pltpu.CompilerParams(
            collective_id=0, has_side_effects=True, vmem_limit_bytes=32 << 20
        ),
    )(
        *(
            pltpu.with_memory_space_constraint(operand, pltpu.HBM)
            for operand in (
                grad_pooled.reshape(batch * tables_all, embed),
                bag_len.T,
                jnp.transpose(lookup_slot, (1, 2, 0)),
                slot_row.reshape(groups, per_peer).T,
                accum,
                weights,
            )
        )
    )
    chunk = min(rows, 128)
    return pl.pallas_call(
        functools.partial(update_kernel, chunk),
        out_shape=(
            jax.ShapeDtypeStruct(weights.shape, F32),
            jax.ShapeDtypeStruct(accum.shape, F32),
        ),
        in_specs=[vmem] * 4,
        out_specs=(anywhere, anywhere),
        scratch_shapes=[
            pltpu.VMEM(weights.shape, F32),
            pltpu.VMEM(accum.shape, F32),
            pltpu.SemaphoreType.DMA,
            pltpu.SemaphoreType.DMA,
        ],
        compiler_params=pltpu.CompilerParams(vmem_limit_bytes=8 << 20),
    )(held, place, deltas, packed)


def solution(mesh):
    placed = (
        P(("grp", "lane"), None, None),
        P(("grp", "lane"), None),
        P("grp", "lane", None),
        P("grp", "lane", None, None),
        P("lane", "grp", None),
        P("lane", "grp"),
    )
    return jax.shard_map(
        functools.partial(per_device, mesh.shape["grp"], mesh.shape["lane"]),
        mesh=mesh,
        in_specs=placed,
        out_specs=(P("lane", "grp", None), P("lane", "grp")),
        check_vma=False,
    )
```
